512 devices in a mesh: blk: 128 (over z_hi, x, y), chan: 4 (over z_lo, core).
Axes of the slice: x: 4, y: 8, z: 8 (z_hi: 4, z_lo: 2; z = z_hi * 2 + z_lo), core: 2. Of those that a mesh axis runs over, the one named last changes fastest.
Arguments:
- positions: float32 [3, 16384], P(None, 'blk'), may hold values from 0 to 256, as said below
- species: int32 [16384], P('blk'), may hold values from 0 to 1
- node_features: float32 [64, 16384], P('chan', 'blk'), may hold values from -6 to 6
- block_mask: int32 [128, 7], P('blk'), may hold values from 0 to 1, as said below
- radial_weight: float32 [8, 64], P(None, 'chan'), may hold values from -2 to 2
- species_embed: float32 [64, 2], P('chan'), may hold values from 0.25 to 1.75
- center_embed: float32 [64, 2], P('chan'), may hold values from 0.25 to 1.75
- mix_weight: float32 [3, 64, 64], replicated, may hold values from -0.75 to 0.75
Outputs:
- descriptors: float32 [3, 64, 16384], P(None, 'chan', 'blk')
The draws below stay inside these ranges and needn't reach their ends.
Inputs may be any that keep to these rules, and one draw needn't show every extreme that they name: `positions`: atom g lies in slab s = g // 128: its first coordinate in [s * 5 / 3, (s + 1) * 5 / 3), the other two in [0, 48). An arbitrary set of kept slab pairs, symmetric between the two slabs of a pair: block_mask[i, 3 + k] equals block_mask[(i + k) mod 128, 3 - k]; the middle column is 1.
All inputs are finite; a program needn't handle non-finite values.
Results may differ from the reference program's by a relative error of at most 0.0035.
Values sent between devices are 32-bit elements; how exact they have to be, the bound alone decides.
A program may use at most 64 MiB of HBM per device.

```python
import math
import jax
import jax.numpy as jnp
from jax import lax

ATOM_DEV = 128
C = 64
NB = 8
HOPS = 3
NSPEC = 2
ATOMS = 16384
N_BLK = 128


slab_width = 5.0 / 3.0


cross_width = 48.0


def draw_positions(key, part):
    base = jax.random.fold_in(key, 11)
    first_key, second_key = jax.random.split(base)
    slab_of = (jnp.arange(ATOMS, dtype=jnp.int32) // ATOM_DEV).astype(jnp.float32)
    fraction = jax.random.uniform(first_key, (ATOMS,), jnp.float32)
    transverse = jax.random.uniform(second_key, (2, ATOMS), jnp.float32) * cross_width
    along = (slab_of + 0.999 * fraction) * slab_width
    return jnp.concatenate([along[None], transverse], axis=0).astype(jnp.float32)


def draw_block_mask(key, part):
    base = jax.random.fold_in(key, 23)
    random_ints = jax.random.randint(base, (N_BLK, HOPS), 0, 4)
    forward = (random_ints > 0).astype(jnp.int32)
    block_rows = jnp.arange(N_BLK, dtype=jnp.int32)
    backward = jnp.stack([forward[(block_rows - step) % N_BLK, step - 1] for step in range(1, HOPS + 1)], axis=1)
    backward_cols = backward[:, ::-1]
    return jnp.concatenate([backward_cols, jnp.ones((N_BLK, 1), jnp.int32), forward], axis=1)


def place_ends(values, rng, least, largest):
    longest = values.shape.index(max(values.shape))
    spots = []
    for shift in (0, 1):
        where = [jax.random.randint(jax.random.fold_in(rng, axis), (), 0, length) for axis, length in enumerate(values.shape)]
        where[longest] = (where[longest] + shift) % values.shape[longest]
        spots.append(tuple(where))
    return values.at[spots[0]].set(least).at[spots[1]].set(largest)


def levels(stream_key, shape, shards, least, high):
    factor_of, own = 1.0, jax.random.fold_in(stream_key, 6)
    for axis_at, shards_of in shards:
        steps = jnp.exp(jax.random.uniform(jax.random.fold_in(own, axis_at), (shards_of,), jnp.float32, least / len(shards), high / len(shards)))
        factor_of = factor_of * jnp.repeat(steps, shape[axis_at] // shards_of).reshape([-1 if axis == axis_at else 1 for axis in range(len(shape))])
    return factor_of


def scatter_about(stream_key, extent, spread, bound, shards=(), held_as=jnp.bfloat16):
    loudness = levels(stream_key, extent, shards, -0.22, 0.18) if shards else 1.0
    values = jax.random.normal(stream_key, extent, jnp.float32) * spread * loudness
    return jnp.minimum(jnp.maximum(values, -bound), bound).astype(held_as)


def setup_inputs(seed: int = 0) -> dict:
    keys = jax.random.split(jax.random.key(seed), 9)
    return {
        "positions": draw_positions(jax.random.fold_in(keys[8], 71), 0),
        "species": place_ends(jax.random.randint(keys[1], (ATOMS,), 0, NSPEC), jax.random.fold_in(keys[1], 1), 0, NSPEC - 1).astype(jnp.int32),
        "node_features": scatter_about(keys[2], (C, ATOMS), 1.0, 6.0, ((0, 4), (1, 128)), jnp.float32),
        "block_mask": draw_block_mask(jax.random.fold_in(keys[8], 71), 0),
        "radial_weight": scatter_about(keys[4], (NB, C), NB ** -0.5, 2.0, ((1, 4),), jnp.float32),
        "species_embed": jnp.clip(1.0 + 0.15 * jax.random.normal(keys[5], (C, NSPEC), jnp.float32), 0.25, 1.75),
        "center_embed": jnp.clip(1.0 + 0.15 * jax.random.normal(keys[6], (C, NSPEC), jnp.float32), 0.25, 1.75),
        "mix_weight": scatter_about(keys[7], (3, C, C), C ** -0.5, 0.75, (), jnp.float32),
    }


slab_width = 5.0 / 3.0
cross_width = 48.0
cut_radius = 5.0
soften = 0.25

def table_of(own_pos, other_pos, box_x, keep_pairs, count):
    separation = other_pos[:, None, :] - own_pos[:, :, None]
    lengths = jnp.array([box_x, cross_width, cross_width], dtype=jnp.float32)[:, None, None]
    separation = separation - lengths * jnp.floor(separation / lengths + 0.5)
    distance = jnp.sqrt(lax.optimization_barrier(jnp.sum(separation * separation, axis=0)) + soften)
    unit_x = separation[0] / distance
    unit_y = separation[1] / distance
    unit_z = separation[2] / distance
    root3 = math.sqrt(3.0)
    root15 = math.sqrt(15.0)
    harmonics = jnp.stack([jnp.ones_like(distance), root3 * unit_x, root3 * unit_y, root3 * unit_z, root15 * unit_x * unit_y, root15 * unit_y * unit_z, 0.5 * math.sqrt(5.0) * (2.0 * unit_z * unit_z - unit_x * unit_x - unit_y * unit_y), root15 * unit_x * unit_z, 0.5 * root15 * (unit_x * unit_x - unit_y * unit_y)])
    scaled = distance / cut_radius
    polynomial = 1.0 - 28.0 * scaled ** 6 + 48.0 * scaled ** 7 - 21.0 * scaled ** 8
    envelope = jnp.where(scaled < 1.0, polynomial, 0.0) * keep_pairs
    orders = jnp.arange(1, count + 1, dtype=jnp.float32)[:, None, None]
    radial = math.sqrt(2.0 / cut_radius) * jnp.sin(orders * (math.pi / cut_radius) * distance[None]) / distance[None] * envelope[None]
    return (radial[:, None] * harmonics[None]).astype(jnp.bfloat16)

def weights_lm(mix_weight):
    return jnp.concatenate([mix_weight[0:1], jnp.repeat(mix_weight[1:2], 3, axis=0), jnp.repeat(mix_weight[2:3], 5, axis=0)], axis=0)

def describe(mixed_tensor):
    squares = mixed_tensor * mixed_tensor
    return jnp.log1p(jnp.stack([squares[:, 0], lax.optimization_barrier(jnp.sum(squares[:, 1:4], axis=1)), lax.optimization_barrier(jnp.sum(squares[:, 4:9], axis=1))]))

def reference(positions, species, node_features, block_mask, radial_weight, species_embed, center_embed, mix_weight):
    box_x = float(N_BLK) * slab_width
    kinds = species_embed.shape[1]
    one_hot = (species[None, :] == jnp.arange(kinds, dtype=jnp.int32)[:, None]).astype(jnp.float32)
    embedded = jnp.dot(species_embed, one_hot, precision=lax.Precision.HIGHEST)
    centre = jnp.dot(center_embed, one_hot, precision=lax.Precision.HIGHEST)
    carried = (radial_weight[:, :, None] * (node_features * embedded)[None]).astype(jnp.bfloat16)
    pos_blocks = positions.reshape(3, N_BLK, ATOM_DEV).transpose(1, 0, 2)
    carried_blocks = carried.reshape(NB, C, N_BLK, ATOM_DEV).transpose(2, 0, 1, 3)
    no_self = 1.0 - jnp.eye(ATOM_DEV, dtype=jnp.float32)

    def one_block(block_id):
        own_pos = pos_blocks[block_id]
        summed = jnp.zeros((C, 9, ATOM_DEV), jnp.float32)
        for offset in range(-HOPS, HOPS + 1):
            neighbour = (block_id + offset) % N_BLK
            active = block_mask[block_id, HOPS + offset].astype(jnp.float32)
            keep_pairs = active * no_self if offset == 0 else active
            pair_table = table_of(own_pos, pos_blocks[neighbour], box_x, keep_pairs, NB)
            summed = summed + jnp.einsum('ncb,nmab->cma', carried_blocks[neighbour].astype(jnp.float32), pair_table.astype(jnp.float32), precision=lax.Precision.HIGHEST)
        return summed
    blocks = lax.map(one_block, jnp.arange(N_BLK, dtype=jnp.int32))
    features = blocks.transpose(1, 2, 0, 3).reshape(C, 9, ATOMS) * centre[:, None, :]
    mixed_tensor = jnp.einsum('mpc,cma->pma', weights_lm(mix_weight), features, precision=lax.Precision.HIGHEST)
    return describe(mixed_tensor)
```

```python
import functools
import math

import jax
import jax.numpy as jnp
from jax import lax
from jax.experimental import pallas as pl
from jax.experimental.pallas import tpu as pltpu
from jax.sharding import PartitionSpec as P

MESH = pl.DeviceIdType.MESH

slab_width = 5.0 / 3.0
cross_width = 48.0
cut_radius = 5.0
soften = 0.25

HOPS = 3
ATOMS = 128
CHANS = 4
CD = 16
C = 64
NB = 8
NM = 9
HALF = 16
BF = jnp.bfloat16
F32 = jnp.float32


def sin_cos(angle):
    x = angle - 0.5 * math.pi
    y = x * x
    even = 2.0876756987868099e-9 * y - 2.755731922398589e-7
    even = even * y + 2.48015873015873e-5
    even = even * y - 1.388888888888889e-3
    even = even * y + 4.1666666666666664e-2
    even = even * y - 0.5
    even = even * y + 1.0
    odd = -2.505210838544172e-8 * y + 2.7557319223985893e-6
    odd = odd * y - 1.984126984126984e-4
    odd = odd * y + 8.333333333333333e-3
    odd = odd * y - 1.6666666666666666e-1
    odd = odd * y * x + x
    return even, -odd


def kernel(
    box_x,
    n_blk,
    pos_hbm,
    spe_hbm,
    fea_hbm,
    msk_hbm,
    rad_hbm,
    sem_hbm,
    cem_hbm,
    mix_hbm,
    out_ref,
    pos,
    spe,
    fea,
    msk,
    rad,
    emb,
    cen,
    mix,
    maskb,
    radb,
    embb,
    tab,
    carr,
    acc,
    lsem,
    fs,
    fr,
    ps,
    pr,
    ss,
    sr,
    gs,
    gr,
    qs,
    qr,
):
    me = lax.axis_index("blk")
    ch = lax.axis_index("chan")
    last = n_blk - HOPS
    late = me >= last
    partner = ch + 1 - 2 * lax.rem(ch, 2)

    def slab(offset):
        return lax.rem(me + offset + n_blk, n_blk)

    def chan(c):
        return lax.rem(ch + c, CHANS)

    def to(offset, c):
        return {"blk": slab(offset), "chan": chan(c)}

    barrier = pltpu.get_barrier_semaphore()

    def greet(offset, c):
        pl.semaphore_signal(barrier, inc=1, device_id=to(offset, c), device_id_type=MESH)

    for c in (1, 2, 3):
        greet(0, c)
    for k in (1, 2, 3):
        greet(-k, 0)
        greet(-k, 2)
    for k in (1, 2, 3):

        @pl.when(me + k < last)
        def _(k=k):
            greet(k, 0)
            greet(k, 2)

    first = [
        pltpu.make_async_copy(pos_hbm, pos.at[HOPS], lsem.at[0]),
        pltpu.make_async_copy(spe_hbm, spe.at[HOPS], lsem.at[1]),
        pltpu.make_async_copy(fea_hbm, fea.at[HOPS, ch], lsem.at[2]),
    ]
    params = [
        pltpu.make_async_copy(rad_hbm, rad.at[ch], lsem.at[3]),
        pltpu.make_async_copy(sem_hbm, emb.at[ch], lsem.at[4]),
        pltpu.make_async_copy(cem_hbm, cen.at[ch], lsem.at[5]),
    ]
    rest = [
        pltpu.make_async_copy(msk_hbm, msk, lsem.at[6]),
        pltpu.make_async_copy(
            mix_hbm.at[:, pl.ds(pl.multiple_of(ch * CD, CD), CD), :], mix, lsem.at[7]
        ),
    ]
    for copy in first + params + rest:
        copy.start()
    for copy in first:
        copy.wait()
    lower = jnp.where(late, 0, jnp.minimum(me, HOPS))
    pl.semaphore_wait(barrier, 3 + 2 * (HOPS + lower))

    def sends(offset):
        slot = HOPS - offset
        out = []
        for c in (0, 2):
            out.append(
                pltpu.make_async_remote_copy(
                    src_ref=fea.at[HOPS, ch],
                    dst_ref=fea.at[slot, ch],
                    send_sem=fs.at[slot, c],
                    recv_sem=fr.at[slot, ch],
                    device_id=to(offset, c),
                    device_id_type=MESH,
                )
            )
        out.append(
            pltpu.make_async_remote_copy(
                src_ref=pos.at[HOPS],
                dst_ref=pos.at[slot],
                send_sem=ps.at[slot],
                recv_sem=pr.at[slot],
                device_id=to(offset, 0),
                device_id_type=MESH,
            )
        )
        out.append(
            pltpu.make_async_remote_copy(
                src_ref=spe.at[HOPS],
                dst_ref=spe.at[slot],
                send_sem=ss.at[slot],
                recv_sem=sr.at[slot],
                device_id=to(offset, 0),
                device_id_type=MESH,
            )
        )
        return out

    for k in (3, 2, 1):
        for copy in sends(k):
            copy.start()
    for k in (1, 2, 3):

        @pl.when(jnp.logical_and(me < last, me >= k))
        def _(k=k):
            for copy in sends(-k):
                copy.start()

    for copy in params:
        copy.wait()
    gathers = []
    for c in (1, 2, 3):
        for q, (ref, sem, got) in enumerate(
            (
                (rad.at[ch], qs.at[0, c], qr.at[0, ch]),
                (emb.at[ch], qs.at[1, c], qr.at[1, ch]),
                (cen.at[ch], qs.at[2, c], qr.at[2, ch]),
                (fea.at[HOPS, ch], gs.at[HOPS, c], gr.at[HOPS, ch]),
            )
        ):
            gathers.append(
                pltpu.make_async_remote_copy(
                    src_ref=ref,
                    dst_ref=ref,
                    send_sem=sem,
                    recv_sem=got,
                    device_id=to(0, c),
                    device_id_type=MESH,
                )
            )
    for copy in gathers:
        copy.start()

    def relays(slot):
        out = []
        for q, c in ((0, 0), (1, 2)):
            a = chan(c)
            out.append(
                pltpu.make_async_remote_copy(
                    src_ref=fea.at[slot, a],
                    dst_ref=fea.at[slot, a],
                    send_sem=gs.at[slot, q],
                    recv_sem=gr.at[slot, a],
                    device_id={"blk": me, "chan": partner},
                    device_id_type=MESH,
                )
            )
        return out

    def arrived(ref, sem):
        pltpu.make_async_remote_copy(
            src_ref=ref,
            dst_ref=ref,
            send_sem=lsem.at[8],
            recv_sem=sem,
            device_id={"blk": me, "chan": partner},
            device_id_type=MESH,
        ).wait_recv()

    for copy in rest:
        copy.wait()
    for s in range(2 * HOPS + 1):
        maskb[s] = jnp.broadcast_to(msk[:, s : s + 1].astype(F32), (8, ATOMS))

    for c in (1, 2, 3):
        a = chan(c)
        arrived(rad.at[a], qr.at[0, a])
        arrived(emb.at[a], qr.at[1, a])
        arrived(cen.at[a], qr.at[2, a])
        arrived(fea.at[HOPS, a], gr.at[HOPS, a])

    eye = lax.broadcasted_iota(jnp.int32, (CD, CD), 0) == lax.broadcasted_iota(
        jnp.int32, (CD, CD), 1
    )
    for q in range(CHANS):
        rows = slice(q * CD, (q + 1) * CD)
        for n in range(NB):
            row = jnp.broadcast_to(rad[q, n : n + 1, :], (CD, CD))
            column = jnp.sum(jnp.where(eye, row, 0.0), axis=1, keepdims=True)
            radb[n, rows, :] = jnp.broadcast_to(column, (CD, ATOMS))
        for kind in (0, 1):
            for at, ref in ((kind, emb), (2 + kind, cen)):
                row = jnp.broadcast_to(ref[q, kind : kind + 1, :], (CD, CD))
                column = jnp.sum(jnp.where(eye, row, 0.0), axis=1, keepdims=True)
                embb[at, rows, :] = jnp.broadcast_to(column, (CD, ATOMS))

    acc[...] = jnp.zeros_like(acc)
    own = pos[HOPS]
    own_x, own_y, own_z = own[0:1], own[1:2], own[2:3]
    lane = lax.broadcasted_iota(jnp.int32, (HALF, ATOMS), 1)
    sublane = lax.broadcasted_iota(jnp.int32, (HALF, ATOMS), 0)
    root3 = math.sqrt(3.0)
    ratio = math.sqrt(5.0 / 3.0)

    def offset_at(t):
        k = lax.rem(t + 2, 3) + 1
        sign = jnp.where(late, -1, 1) * jnp.where(t <= 3, 1, -1)
        return jnp.where(t == 0, 0, sign * k)

    def fetch(t):
        offset = offset_at(t)
        slot = offset + HOPS
        arrived(pos.at[slot], pr.at[slot])
        arrived(spe.at[slot], sr.at[slot])
        for c in (0, 2):
            a = chan(c)
            arrived(fea.at[slot, a], fr.at[slot, a])
        for copy in relays(slot):
            copy.start()
        k = lax.rem(t + 2, 3) + 1
        early = jnp.logical_and(me < last, me >= k)

        @pl.when(jnp.logical_and(offset < 0, jnp.logical_not(early)))
        def _():
            for copy in sends(offset):
                copy.start()

    def pairs(slot, apart):
        kinds = jnp.broadcast_to(spe[slot], (C, ATOMS)) == 1
        embedded = jnp.where(kinds, embb[1], embb[0])
        scaled = fea[slot].reshape(C, ATOMS) * embedded
        for n in range(NB):
            carr[:, n * ATOMS : (n + 1) * ATOMS] = (radb[n] * scaled).astype(BF)
        other = jnp.concatenate([pos[slot], jnp.zeros((5, ATOMS), F32)], axis=0)
        columns = jnp.transpose(other)
        keep = maskb[slot]
        keep = jnp.concatenate([keep, keep], axis=0)
        for tile in range(ATOMS // HALF):
            rows = slice(tile * HALF, (tile + 1) * HALF)
            dx = columns[rows, 0:1] - own_x
            dy = columns[rows, 1:2] - own_y
            dz = columns[rows, 2:3] - own_z
            dx = dx - box_x * jnp.floor(dx * (1.0 / box_x) + 0.5)
            dy = dy - cross_width * jnp.floor(dy * (1.0 / cross_width) + 0.5)
            dz = dz - cross_width * jnp.floor(dz * (1.0 / cross_width) + 0.5)
            square = dx * dx + dy * dy + dz * dz + soften
            inverse = lax.rsqrt(square)
            distance = square * inverse
            short = jnp.minimum(distance, cut_radius)
            x = short * (1.0 / cut_radius)
            x2 = x * x
            inner = x * (48.0 - 21.0 * x) - 28.0
            envelope = jnp.where(distance < cut_radius, 1.0 + x2 * x2 * x2 * inner, 0.0)
            same = (sublane + tile * HALF) == (lane + apart)
            amplitude = jnp.where(
                same, 0.0, (math.sqrt(2.0 / cut_radius) * inverse) * (envelope * keep)
            )
            sine, cosine = sin_cos(short * (math.pi / cut_radius))
            twice = 2.0 * cosine
            radial = [amplitude * sine]
            radial.append(twice * radial[0])
            for n in range(2, NB):
                radial.append(twice * radial[n - 1] - radial[n - 2])
            scale = inverse * root3
            hx, hy, hz = dx * scale, dy * scale, dz * scale
            gx, gy = ratio * hx, ratio * hy
            xx, yy = gx * hx, gy * hy
            zz = (2.0 * ratio) * (hz * hz)
            harmonics = [
                None,
                hx,
                hy,
                hz,
                gx * hy,
                gy * hz,
                (0.5 / root3) * (zz - xx - yy),
                gx * hz,
                0.5 * (xx - yy),
            ]
            for n in range(NB):
                at = slice(n * ATOMS + tile * HALF, n * ATOMS + (tile + 1) * HALF)
                for m in range(NM):
                    value = radial[n] if m == 0 else radial[n] * harmonics[m]
                    tab[at, m * ATOMS : (m + 1) * ATOMS] = value.astype(BF)
        acc[...] += jnp.dot(carr[...], tab[...], preferred_element_type=F32)

    def step(t, carry):
        @pl.when(t < 2 * HOPS)
        def _():
            fetch(t + 1)

        slot = offset_at(t) + HOPS

        @pl.when(t > 0)
        def _():
            for c in (1, 3):
                a = chan(c)
                arrived(fea.at[slot, a], gr.at[slot, a])

        pairs(slot, jnp.where(t == 0, 0, 2 * ATOMS))
        return carry

    lax.fori_loop(0, 2 * HOPS + 1, step, 0)

    kinds = jnp.broadcast_to(spe[HOPS], (C, ATOMS)) == 1
    centre = jnp.where(kinds, embb[3], embb[2])
    order_of = (0, 1, 1, 1, 2, 2, 2, 2, 2)
    sums = [None, None, None]
    weights = []
    for order in range(3):
        w = mix[order]
        high = w.astype(BF)
        low = (w - high.astype(F32)).astype(BF)
        weights.append((high, low))
    for m in range(NM):
        f = acc[:, m * ATOMS : (m + 1) * ATOMS] * centre
        high = f.astype(BF)
        low = (f - high.astype(F32)).astype(BF)
        w_high, w_low = weights[order_of[m]]
        mixed = (
            jnp.dot(w_high, high, preferred_element_type=F32)
            + jnp.dot(w_low, high, preferred_element_type=F32)
            + jnp.dot(w_high, low, preferred_element_type=F32)
        )
        square = mixed * mixed
        order = order_of[m]
        sums[order] = square if sums[order] is None else sums[order] + square
    for order in range(3):
        out_ref[order] = sums[order]

    for k in (1, 2, 3):
        for offset in (k, -k):
            for copy in sends(offset):
                copy.wait_send()
            for copy in relays(offset + HOPS):
                copy.wait_send()
    for copy in gathers:
        copy.wait_send()


def shards(
    positions,
    species,
    node_features,
    block_mask,
    radial_weight,
    species_embed,
    center_embed,
    mix_weight,
):
    n_blk = lax.axis_size("blk")
    box_x = float(n_blk) * slab_width
    dma = pltpu.SemaphoreType.DMA
    slots = 2 * HOPS + 1
    vmem = pltpu.VMEM
    sums = pl.pallas_call(
        functools.partial(kernel, box_x, n_blk),
        name="pair_descriptor",
        out_shape=jax.ShapeDtypeStruct((3, CD, ATOMS), F32),
        in_specs=[pl.BlockSpec(memory_space=pl.ANY)] * 8,
        out_specs=pl.BlockSpec(memory_space=pltpu.VMEM),
        scratch_shapes=[
            vmem((slots, 3, ATOMS), F32),
            vmem((slots, 1, ATOMS), jnp.int32),
            vmem((slots, CHANS, CD, ATOMS), F32),
            vmem((1, slots), jnp.int32),
            vmem((CHANS, NB, CD), F32),
            vmem((CHANS, 2, CD), F32),
            vmem((CHANS, 2, CD), F32),
            vmem((3, CD, C), F32),
            vmem((slots, 8, ATOMS), F32),
            vmem((NB, C, ATOMS), F32),
            vmem((4, C, ATOMS), F32),
            vmem((NB * ATOMS, NM * ATOMS), BF),
            vmem((C, NB * ATOMS), BF),
            vmem((C, NM * ATOMS), F32),
            dma((9,)),
            dma((slots, CHANS)),
            dma((slots, CHANS)),
            dma((slots,)),
            dma((slots,)),
            dma((slots,)),
            dma((slots,)),
            dma((slots, CHANS)),
            dma((slots, CHANS)),
            dma((3, CHANS)),
            dma((3, CHANS)),
        ],
        compiler_params=pltpu.CompilerParams(collective_id=0, has_side_effects=True),
    )(
        positions,
        species.reshape(1, ATOMS),
        node_features,
        block_mask,
        radial_weight,
        species_embed.T,
        center_embed.T,
        mix_weight,
    )
    return jnp.log1p(sums)


def solution(mesh):
    return jax.shard_map(
        shards,
        mesh=mesh,
        in_specs=(
            P(None, "blk"),
            P("blk"),
            P("chan", "blk"),
            P("blk", None),
            P(None, "chan"),
            P("chan", None),
            P("chan", None),
            P(),
        ),
        out_specs=P(None, "chan", "blk"),
        check_vma=False,
    )
```

```python
import functools
import math

import jax
import jax.numpy as jnp
from jax import lax
from jax.experimental import pallas as pl
from jax.experimental.pallas import tpu as pltpu
from jax.sharding import PartitionSpec as P

MESH = pl.DeviceIdType.MESH

slab_width = 5.0 / 3.0
cross_width = 48.0
cut_radius = 5.0
soften = 0.25

HOPS = 3
ATOMS = 128
CHANS = 4
CD = 16
C = 64
NB = 8
NM = 9
HALF = 16
BF = jnp.bfloat16
F32 = jnp.float32


def sin_cos(angle):
    x = angle - 0.5 * math.pi
    y = x * x
    even = 2.0876756987868099e-9 * y - 2.755731922398589e-7
    even = even * y + 2.48015873015873e-5
    even = even * y - 1.388888888888889e-3
    even = even * y + 4.1666666666666664e-2
    even = even * y - 0.5
    even = even * y + 1.0
    odd = -2.505210838544172e-8 * y + 2.7557319223985893e-6
    odd = odd * y - 1.984126984126984e-4
    odd = odd * y + 8.333333333333333e-3
    odd = odd * y - 1.6666666666666666e-1
    odd = odd * y * x + x
    return even, -odd


def kernel(
    box_x,
    n_blk,
    row,
    pos_hbm,
    spe_hbm,
    fea_hbm,
    msk_hbm,
    rad_hbm,
    sem_hbm,
    cem_hbm,
    mix_hbm,
    out_ref,
    pos,
    spe,
    fea,
    msk,
    rad,
    emb,
    cen,
    mix,
    maskb,
    radb,
    embb,
    tab_a,
    tab_b,
    carr,
    acc,
    lsem,
    fs,
    fr,
    ps,
    pr,
    ss,
    sr,
    gr,
    qs,
    qr,
):
    me = lax.axis_index("blk")
    ch = lax.axis_index("chan")
    last = n_blk - HOPS
    late = me >= last
    side = jnp.where(lax.rem(me, row) < row // 2, 1, -1)
    partner = ch + 1 - 2 * lax.rem(ch, 2)

    def slab(offset):
        return lax.rem(me + offset + n_blk, n_blk)

    def chan(c):
        return lax.rem(ch + c, CHANS)

    def to(offset, c):
        return {"blk": slab(offset), "chan": chan(c)}

    barrier = pltpu.get_barrier_semaphore()

    def greet(offset, c):
        pl.semaphore_signal(barrier, inc=1, device_id=to(offset, c), device_id_type=MESH)

    first = [
        pltpu.make_async_copy(pos_hbm, pos.at[HOPS], lsem.at[0]),
        pltpu.make_async_copy(spe_hbm, spe.at[HOPS], lsem.at[1]),
        pltpu.make_async_copy(fea_hbm, fea.at[HOPS, ch], lsem.at[2]),
    ]
    params = [
        pltpu.make_async_copy(rad_hbm, rad.at[ch], lsem.at[3]),
        pltpu.make_async_copy(sem_hbm, emb.at[ch], lsem.at[4]),
        pltpu.make_async_copy(cem_hbm, cen.at[ch], lsem.at[5]),
    ]
    rest = [
        pltpu.make_async_copy(msk_hbm, msk, lsem.at[6]),
        pltpu.make_async_copy(
            mix_hbm.at[:, pl.ds(pl.multiple_of(ch * CD, CD), CD), :], mix, lsem.at[7]
        ),
    ]
    for copy in first:
        copy.start()

    ahead = jnp.logical_and(late, ch < 2)

    def apart_in_z(c):
        return chan(c) // 2 != ch // 2

    for k in (3, 2, 1):
        greet(-k, 0)
        greet(-k, 2)
    for c in (1, 2, 3):

        @pl.when(jnp.logical_not(jnp.logical_and(late, jnp.logical_and(ch >= 2, apart_in_z(c)))))
        def _(c=c):
            greet(0, c)

    for k in (1, 2, 3):

        @pl.when(me + k < last + (k >= HOPS))
        def _(k=k):
            greet(k, 0)
            greet(k, 2)

    for copy in params + rest:
        copy.start()
    for copy in first:
        copy.wait()
    lower = jnp.where(late, jnp.where(me == last, 1, 0), jnp.minimum(me, HOPS))
    pl.semaphore_wait(barrier, jnp.where(ahead, 1, 3) + 2 * (HOPS + lower))

    def sends(offset):
        slot = HOPS - offset
        out = []
        for c in (0, 2):
            out.append(
                pltpu.make_async_remote_copy(
                    src_ref=fea.at[HOPS, ch],
                    dst_ref=fea.at[slot, ch],
                    send_sem=fs,
                    recv_sem=fr.at[slot, ch],
                    device_id=to(offset, c),
                    device_id_type=MESH,
                )
            )
        out.append(
            pltpu.make_async_remote_copy(
                src_ref=pos.at[HOPS],
                dst_ref=pos.at[slot],
                send_sem=ps,
                recv_sem=pr.at[slot],
                device_id=to(offset, 0),
                device_id_type=MESH,
            )
        )
        out.append(
            pltpu.make_async_remote_copy(
                src_ref=spe.at[HOPS],
                dst_ref=spe.at[slot],
                send_sem=ss,
                recv_sem=sr.at[slot],
                device_id=to(offset, 0),
                device_id_type=MESH,
            )
        )
        return out

    nearest = jnp.where(late, n_blk - me, HOPS)
    for turn in range(HOPS):
        k = nearest + turn
        for copy in sends(jnp.where(k > HOPS, k - HOPS, k)):
            copy.start()
    def early(k):
        return jnp.logical_and(me >= k, me < jnp.where(k >= HOPS, last + 1, last))

    for k in (1, 2, 3):

        @pl.when(early(k))
        def _(k=k):
            for copy in sends(-k):
                copy.start()

    for copy in params:
        copy.wait()

    def gathers(c):
        out = []
        for ref, sem, got in (
            (rad.at[ch], qs.at[0], qr.at[0, ch]),
            (emb.at[ch], qs.at[1], qr.at[1, ch]),
            (cen.at[ch], qs.at[2], qr.at[2, ch]),
            (fea.at[HOPS, ch], fs, gr.at[HOPS, ch]),
        ):
            out.append(
                pltpu.make_async_remote_copy(
                    src_ref=ref,
                    dst_ref=ref,
                    send_sem=sem,
                    recv_sem=got,
                    device_id=to(0, c),
                    device_id_type=MESH,
                )
            )
        return out

    for c in (1, 2, 3):

        @pl.when(jnp.logical_not(jnp.logical_and(ahead, apart_in_z(c))))
        def _(c=c):
            for copy in gathers(c):
                copy.start()

    def relays(slot):
        out = []
        for q, c in ((0, 0), (1, 2)):
            a = chan(c)
            out.append(
                pltpu.make_async_remote_copy(
                    src_ref=fea.at[slot, a],
                    dst_ref=fea.at[slot, a],
                    send_sem=fs,
                    recv_sem=gr.at[slot, a],
                    device_id={"blk": me, "chan": partner},
                    device_id_type=MESH,
                )
            )
        return out

    def arrived(ref, sem):
        pltpu.make_async_remote_copy(
            src_ref=ref,
            dst_ref=ref,
            send_sem=lsem.at[8],
            recv_sem=sem,
            device_id={"blk": me, "chan": partner},
            device_id_type=MESH,
        ).wait_recv()

    for copy in rest:
        copy.wait()
    for s in range(2 * HOPS + 1):
        maskb[s] = jnp.broadcast_to(msk[:, s : s + 1].astype(F32), (8, ATOMS))

    for c in (1, 2, 3):
        a = chan(c)
        arrived(rad.at[a], qr.at[0, a])
        arrived(emb.at[a], qr.at[1, a])
        arrived(cen.at[a], qr.at[2, a])
        arrived(fea.at[HOPS, a], gr.at[HOPS, a])

        @pl.when(jnp.logical_and(ahead, apart_in_z(c)))
        def _(c=c):
            for copy in gathers(c):
                copy.start()

    eye = lax.broadcasted_iota(jnp.int32, (CD, CD), 0) == lax.broadcasted_iota(
        jnp.int32, (CD, CD), 1
    )
    for q in range(CHANS):
        rows = slice(q * CD, (q + 1) * CD)
        for n in range(NB):
            row = jnp.broadcast_to(rad[q, n : n + 1, :], (CD, CD))
            column = jnp.sum(jnp.where(eye, row, 0.0), axis=1, keepdims=True)
            radb[n, rows, :] = jnp.broadcast_to(column, (CD, ATOMS))
        for kind in (0, 1):
            for at, ref in ((kind, emb), (2 + kind, cen)):
                row = jnp.broadcast_to(ref[q, kind : kind + 1, :], (CD, CD))
                column = jnp.sum(jnp.where(eye, row, 0.0), axis=1, keepdims=True)
                embb[at, rows, :] = jnp.broadcast_to(column, (CD, ATOMS))

    acc[...] = jnp.zeros_like(acc)
    own = pos[HOPS]
    own_x, own_y, own_z = own[0:1], own[1:2], own[2:3]
    lane = lax.broadcasted_iota(jnp.int32, (HALF, ATOMS), 1)
    sublane = lax.broadcasted_iota(jnp.int32, (HALF, ATOMS), 0)
    root3 = math.sqrt(3.0)
    ratio = math.sqrt(5.0 / 3.0)

    def offset_at(t):
        k = lax.rem(t + 2, 3) + 1
        return jnp.where(t == 0, 0, jnp.where(t <= HOPS, side, -side) * k)

    def fetch(t):
        offset = offset_at(t)
        slot = offset + HOPS
        arrived(pos.at[slot], pr.at[slot])
        arrived(spe.at[slot], sr.at[slot])
        for c in (0, 2):
            a = chan(c)
            arrived(fea.at[slot, a], fr.at[slot, a])
        for copy in relays(slot):
            copy.start()
        k = lax.rem(t + 2, 3) + 1

        @pl.when(jnp.logical_and(offset < 0, jnp.logical_not(early(k))))
        def _():
            for copy in sends(offset):
                copy.start()

    def weigh(slot, tab):
        kinds = jnp.broadcast_to(spe[slot], (C, ATOMS)) == 1
        embedded = jnp.where(kinds, embb[1], embb[0])
        scaled = fea[slot].reshape(C, ATOMS) * embedded
        for n in range(NB):
            carr[:, n * ATOMS : (n + 1) * ATOMS] = (radb[n] * scaled).astype(BF)
        acc[...] += jnp.dot(carr[...], tab[...], preferred_element_type=F32)

    def table(slot, apart, tab):
        other = jnp.concatenate([pos[slot], jnp.zeros((5, ATOMS), F32)], axis=0)
        columns = jnp.transpose(other)
        keep = maskb[slot]
        keep = jnp.concatenate([keep, keep], axis=0)
        for tile in range(ATOMS // HALF):
            rows = slice(tile * HALF, (tile + 1) * HALF)
            dx = columns[rows, 0:1] - own_x
            dy = columns[rows, 1:2] - own_y
            dz = columns[rows, 2:3] - own_z
            dx = dx - box_x * jnp.floor(dx * (1.0 / box_x) + 0.5)
            dy = dy - cross_width * jnp.floor(dy * (1.0 / cross_width) + 0.5)
            dz = dz - cross_width * jnp.floor(dz * (1.0 / cross_width) + 0.5)
            square = dx * dx + dy * dy + dz * dz + soften
            inverse = lax.rsqrt(square)
            distance = square * inverse
            short = jnp.minimum(distance, cut_radius)
            x = short * (1.0 / cut_radius)
            x2 = x * x
            inner = x * (48.0 - 21.0 * x) - 28.0
            envelope = jnp.where(distance < cut_radius, 1.0 + x2 * x2 * x2 * inner, 0.0)
            same = (sublane + tile * HALF) == (lane + apart)
            amplitude = jnp.where(
                same, 0.0, (math.sqrt(2.0 / cut_radius) * inverse) * (envelope * keep)
            )
            sine, cosine = sin_cos(short * (math.pi / cut_radius))
            twice = 2.0 * cosine
            radial = [amplitude * sine]
            radial.append(twice * radial[0])
            for n in range(2, NB):
                radial.append(twice * radial[n - 1] - radial[n - 2])
            scale = inverse * root3
            hx, hy, hz = dx * scale, dy * scale, dz * scale
            gx, gy = ratio * hx, ratio * hy
            xx, yy = gx * hx, gy * hy
            zz = (2.0 * ratio) * (hz * hz)
            harmonics = [
                None,
                hx,
                hy,
                hz,
                gx * hy,
                gy * hz,
                (0.5 / root3) * (zz - xx - yy),
                gx * hz,
                0.5 * (xx - yy),
            ]
            for n in range(NB):
                at = slice(n * ATOMS + tile * HALF, n * ATOMS + (tile + 1) * HALF)
                for m in range(NM):
                    value = radial[n] if m == 0 else radial[n] * harmonics[m]
                    tab[at, m * ATOMS : (m + 1) * ATOMS] = value.astype(BF)

    def swapped(t):
        slot = offset_at(t) + HOPS

        @pl.when(t > 0)
        def _():
            for c in (1, 3):
                a = chan(c)
                arrived(fea.at[slot, a], gr.at[slot, a])

        return slot

    def advance(t, tab, other_tab):
        fetch(t + 1)
        slot = swapped(t)
        weigh(slot, tab)
        table(offset_at(t + 1) + HOPS, 2 * ATOMS, other_tab)

    def finish(t, tab):
        weigh(swapped(t), tab)

    def side_of(i, carry):
        t = i * (HOPS + 1)

        @pl.when(i > 0)
        def _():
            fetch(t)

        table(offset_at(t) + HOPS, jnp.where(i == 0, 0, 2 * ATOMS), tab_a)
        advance(t, tab_a, tab_b)
        advance(t + 1, tab_b, tab_a)

        @pl.when(i == 0)
        def _():
            advance(t + 2, tab_a, tab_b)
            finish(t + 3, tab_b)

        @pl.when(i > 0)
        def _():
            finish(t + 2, tab_a)

        return carry

    lax.fori_loop(0, 2, side_of, 0)

    def sent(ref, sem):
        pltpu.make_async_remote_copy(
            src_ref=ref,
            dst_ref=ref,
            send_sem=sem,
            recv_sem=lsem.at[8],
            device_id={"blk": me, "chan": partner},
            device_id_type=MESH,
        ).wait_send()

    sent(fea.at[0 : 2 * HOPS], fs)
    sent(fea.at[0, 0:3], fs)
    sent(pos.at[0 : 2 * HOPS], ps)
    sent(spe.at[0 : 2 * HOPS], ss)
    sent(rad.at[0:3], qs.at[0])
    sent(emb.at[0:3], qs.at[1])
    sent(cen.at[0:3], qs.at[2])

    kinds = jnp.broadcast_to(spe[HOPS], (C, ATOMS)) == 1
    centre = jnp.where(kinds, embb[3], embb[2])
    order_of = (0, 1, 1, 1, 2, 2, 2, 2, 2)
    sums = [None, None, None]
    weights = []
    for order in range(3):
        w = mix[order]
        high = w.astype(BF)
        low = (w - high.astype(F32)).astype(BF)
        weights.append((high, low))
    for m in range(NM):
        f = acc[:, m * ATOMS : (m + 1) * ATOMS] * centre
        high = f.astype(BF)
        low = (f - high.astype(F32)).astype(BF)
        w_high, w_low = weights[order_of[m]]
        mixed = (
            jnp.dot(w_high, high, preferred_element_type=F32)
            + jnp.dot(w_low, high, preferred_element_type=F32)
            + jnp.dot(w_high, low, preferred_element_type=F32)
        )
        square = mixed * mixed
        order = order_of[m]
        sums[order] = square if sums[order] is None else sums[order] + square
    for order in range(3):
        out_ref[order] = sums[order]


def shards(
    positions,
    species,
    node_features,
    block_mask,
    radial_weight,
    species_embed,
    center_embed,
    mix_weight,
):
    n_blk = lax.axis_size("blk")
    box_x = float(n_blk) * slab_width
    dma = pltpu.SemaphoreType.DMA
    slots = 2 * HOPS + 1
    vmem = pltpu.VMEM
    sums = pl.pallas_call(
        functools.partial(kernel, box_x, n_blk, 8),
        name="pair_descriptor",
        out_shape=pltpu.VMEM((3, CD, ATOMS), F32),
        in_specs=[pl.BlockSpec(memory_space=pl.ANY)] * 8,
        out_specs=pl.BlockSpec(memory_space=pltpu.VMEM),
        scratch_shapes=[
            vmem((slots, 3, ATOMS), F32),
            vmem((slots, 1, ATOMS), jnp.int32),
            vmem((slots, CHANS, CD, ATOMS), F32),
            vmem((1, slots), jnp.int32),
            vmem((CHANS, NB, CD), F32),
            vmem((CHANS, 2, CD), F32),
            vmem((CHANS, 2, CD), F32),
            vmem((3, CD, C), F32),
            vmem((slots, 8, ATOMS), F32),
            vmem((NB, C, ATOMS), F32),
            vmem((4, C, ATOMS), F32),
            vmem((NB * ATOMS, NM * ATOMS), BF),
            vmem((NB * ATOMS, NM * ATOMS), BF),
            vmem((C, NB * ATOMS), BF),
            vmem((C, NM * ATOMS), F32),
            dma((9,)),
            dma(()),
            dma((slots, CHANS)),
            dma(()),
            dma((slots,)),
            dma(()),
            dma((slots,)),
            dma((slots, CHANS)),
            dma((3,)),
            dma((3, CHANS)),
        ],
        compiler_params=pltpu.CompilerParams(collective_id=0, has_side_effects=True),
    )(
        positions,
        species.reshape(1, ATOMS),
        node_features,
        block_mask,
        radial_weight,
        species_embed.T,
        center_embed.T,
        mix_weight,
    )
    return jnp.log1p(sums)


def solution(mesh):
    return jax.shard_map(
        shards,
        mesh=mesh,
        in_specs=(
            P(None, "blk"),
            P("blk"),
            P("chan", "blk"),
            P("blk", None),
            P(None, "chan"),
            P("chan", None),
            P("chan", None),
            P(),
        ),
        out_specs=P(None, "chan", "blk"),
        check_vma=False,
    )
```

```python
import functools
import math

import jax
import jax.numpy as jnp
from jax import lax
from jax.experimental import pallas as pl
from jax.experimental.pallas import tpu as pltpu
from jax.sharding import PartitionSpec as P

MESH = pl.DeviceIdType.MESH

slab_width = 5.0 / 3.0
cross_width = 48.0
cut_radius = 5.0
soften = 0.25

HOPS = 3
ATOMS = 128
CHANS = 4
CD = 16
C = 64
NB = 8
NM = 9
HALF = 16
PIECES = 5
BF = jnp.bfloat16
F32 = jnp.float32


def sin_cos(angle):
    x = angle - 0.5 * math.pi
    y = x * x
    even = 2.0876756987868099e-9 * y - 2.755731922398589e-7
    even = even * y + 2.48015873015873e-5
    even = even * y - 1.388888888888889e-3
    even = even * y + 4.1666666666666664e-2
    even = even * y - 0.5
    even = even * y + 1.0
    odd = -2.505210838544172e-8 * y + 2.7557319223985893e-6
    odd = odd * y - 1.984126984126984e-4
    odd = odd * y + 8.333333333333333e-3
    odd = odd * y - 1.6666666666666666e-1
    odd = odd * y * x + x
    return even, -odd


def kernel(
    box_x,
    n_blk,
    row,
    pos_hbm,
    spe_hbm,
    fea_hbm,
    msk_hbm,
    rad_hbm,
    sem_hbm,
    cem_hbm,
    mix_hbm,
    out_ref,
    pos,
    spe,
    fea,
    msk,
    prm,
    mix,
    maskb,
    radb,
    embb,
    tab_a,
    tab_b,
    carr,
    acc,
    lsem,
    fs,
    fr,
    ps,
    pr,
    ss,
    sr,
    qs,
    qr,
):
    me = lax.axis_index("blk")
    ch = lax.axis_index("chan")
    last = n_blk - HOPS
    late = me >= last
    side = jnp.where(lax.rem(me, row) < row // 2, 1, -1)
    partner = ch + 1 - 2 * lax.rem(ch, 2)

    def slab(offset):
        return lax.rem(me + offset + n_blk, n_blk)

    def chan(c):
        return lax.rem(ch + c, CHANS)

    def to(offset, c):
        return {"blk": slab(offset), "chan": chan(c)}

    barrier = pltpu.get_barrier_semaphore()

    def greet(offset, c):
        pl.semaphore_signal(barrier, inc=1, device_id=to(offset, c), device_id_type=MESH)

    first = [
        pltpu.make_async_copy(pos_hbm, pos.at[HOPS], lsem.at[0]),
        pltpu.make_async_copy(spe_hbm, spe.at[HOPS], lsem.at[1]),
        pltpu.make_async_copy(fea_hbm, fea.at[HOPS, ch], lsem.at[2]),
    ]
    params = [
        pltpu.make_async_copy(rad_hbm, prm.at[ch, 0], lsem.at[3]),
        pltpu.make_async_copy(sem_hbm, prm.at[ch, 1, 0:2], lsem.at[4]),
        pltpu.make_async_copy(cem_hbm, prm.at[ch, 2, 0:2], lsem.at[5]),
    ]
    rest = [
        pltpu.make_async_copy(msk_hbm, msk, lsem.at[6]),
        pltpu.make_async_copy(
            mix_hbm.at[:, pl.ds(pl.multiple_of(ch * CD, CD), CD), :], mix, lsem.at[7]
        ),
    ]
    for copy in first:
        copy.start()

    directs = jnp.logical_and(late, lax.rem(ch, 2) == 0)
    spared = jnp.logical_and(me == 0, ch == 0)

    ahead = jnp.logical_and(late, ch < 2)

    def apart_in_z(c):
        return chan(c) // 2 != ch // 2

    for k in (3, 2, 1):
        greet(-k, 0)
        greet(-k, 2)

    @pl.when(jnp.logical_and(me == 0, ch == 1))
    def _():
        for k in (3, 2, 1):
            greet(-k, 1)
            greet(-k, 3)

    for c in (1, 2, 3):

        @pl.when(jnp.logical_not(jnp.logical_and(late, jnp.logical_and(ch >= 2, apart_in_z(c)))))
        def _(c=c):
            greet(0, c)

    for k in (1, 2, 3):

        @pl.when(me + k < last + (k >= HOPS))
        def _(k=k):
            greet(k, 0)
            greet(k, 2)

    for copy in params + rest:
        copy.start()
    for copy in first:
        copy.wait()
    lower = jnp.where(late, jnp.where(me == last, 1, 0), jnp.minimum(me, HOPS))
    pl.semaphore_wait(barrier, jnp.where(ahead, 1, 3) + 2 * (HOPS + lower) + directs.astype(jnp.int32))

    def sends(offset):
        slot = HOPS - offset
        out = []
        for c in (0, 2):
            out.append(
                pltpu.make_async_remote_copy(
                    src_ref=fea.at[HOPS, ch],
                    dst_ref=fea.at[slot, ch],
                    send_sem=fs,
                    recv_sem=fr.at[slot, 0],
                    device_id=to(offset, c),
                    device_id_type=MESH,
                )
            )
        out.append(
            pltpu.make_async_remote_copy(
                src_ref=pos.at[HOPS],
                dst_ref=pos.at[slot],
                send_sem=ps,
                recv_sem=pr.at[slot],
                device_id=to(offset, 0),
                device_id_type=MESH,
            )
        )
        out.append(
            pltpu.make_async_remote_copy(
                src_ref=spe.at[HOPS],
                dst_ref=spe.at[slot],
                send_sem=ss,
                recv_sem=sr.at[slot],
                device_id=to(offset, 0),
                device_id_type=MESH,
            )
        )
        return out

    nearest = jnp.where(late, n_blk - me, HOPS)

    def direct():
        return pltpu.make_async_remote_copy(
            src_ref=fea.at[HOPS, ch],
            dst_ref=fea.at[HOPS - nearest, ch],
            send_sem=fs,
            recv_sem=fr.at[HOPS - nearest, 1],
            device_id={"blk": 0, "chan": 1},
            device_id_type=MESH,
        )

    @pl.when(directs)
    def _():
        direct().start()

    for turn in range(HOPS):
        k = nearest + turn
        for copy in sends(jnp.where(k > HOPS, k - HOPS, k)):
            copy.start()
    def early(k):
        return jnp.logical_and(me >= k, me < jnp.where(k >= HOPS, last + 1, last))

    for k in (1, 2, 3):

        @pl.when(early(k))
        def _(k=k):
            for copy in sends(-k):
                copy.start()

    for copy in params:
        copy.wait()

    def gathers(c):
        out = []
        for ref, sem, got in (
            (prm.at[ch], qs, qr),
            (fea.at[HOPS, ch], fs, fr.at[HOPS, 0]),
        ):
            out.append(
                pltpu.make_async_remote_copy(
                    src_ref=ref,
                    dst_ref=ref,
                    send_sem=sem,
                    recv_sem=got,
                    device_id=to(0, c),
                    device_id_type=MESH,
                )
            )
        return out

    for c in (1, 2, 3):

        @pl.when(jnp.logical_not(jnp.logical_and(ahead, apart_in_z(c))))
        def _(c=c):
            for copy in gathers(c):
                copy.start()

    def relays(slot):
        out = []
        for q, c in ((0, 0), (1, 2)):
            a = chan(c)
            out.append(
                pltpu.make_async_remote_copy(
                    src_ref=fea.at[slot, a],
                    dst_ref=fea.at[slot, a],
                    send_sem=fs,
                    recv_sem=fr.at[slot, 1],
                    device_id={"blk": me, "chan": partner},
                    device_id_type=MESH,
                )
            )
        return out

    def arrived(ref, sem):
        pltpu.make_async_remote_copy(
            src_ref=ref,
            dst_ref=ref,
            send_sem=lsem.at[8],
            recv_sem=sem,
            device_id={"blk": me, "chan": partner},
            device_id_type=MESH,
        ).wait_recv()

    for copy in rest:
        copy.wait()
    for s in range(2 * HOPS + 1):
        maskb[s] = jnp.broadcast_to(msk[:, s : s + 1].astype(F32), (8, ATOMS))

    arrived(prm.at[0:3], qr)
    arrived(fea.at[0, 0:3], fr.at[HOPS, 0])
    for c in (1, 2, 3):

        @pl.when(jnp.logical_and(ahead, apart_in_z(c)))
        def _(c=c):
            for copy in gathers(c):
                copy.start()

    eye = lax.broadcasted_iota(jnp.int32, (CD, CD), 0) == lax.broadcasted_iota(
        jnp.int32, (CD, CD), 1
    )
    for q in range(CHANS):
        rows = slice(q * CD, (q + 1) * CD)
        for n in range(NB):
            row = jnp.broadcast_to(prm[q, 0, n : n + 1, :], (CD, CD))
            column = jnp.sum(jnp.where(eye, row, 0.0), axis=1, keepdims=True)
            radb[n, rows, :] = jnp.broadcast_to(column, (CD, ATOMS))
        for kind in (0, 1):
            for at, of in ((kind, 1), (2 + kind, 2)):
                row = jnp.broadcast_to(prm[q, of, kind : kind + 1, :], (CD, CD))
                column = jnp.sum(jnp.where(eye, row, 0.0), axis=1, keepdims=True)
                embb[at, rows, :] = jnp.broadcast_to(column, (CD, ATOMS))

    acc[...] = jnp.zeros_like(acc)
    own = pos[HOPS]
    own_x, own_y, own_z = own[0:1], own[1:2], own[2:3]
    lane = lax.broadcasted_iota(jnp.int32, (HALF, ATOMS), 1)
    sublane = lax.broadcasted_iota(jnp.int32, (HALF, ATOMS), 0)
    root3 = math.sqrt(3.0)
    ratio = math.sqrt(5.0 / 3.0)

    def reach_at(t):
        return jnp.where(jnp.logical_and(late, t <= HOPS), HOPS + 1 - t, lax.rem(t + 2, 3) + 1)

    def offset_at(t):
        k = reach_at(t)
        return jnp.where(t == 0, 0, jnp.where(t <= HOPS, side, -side) * k)

    def fetch(t):
        offset = offset_at(t)
        slot = offset + HOPS
        arrived(pos.at[slot], pr.at[slot])
        arrived(spe.at[slot], sr.at[slot])
        arrived(fea.at[0, 0:2], fr.at[slot, 0])

        @pl.when(jnp.logical_not(jnp.logical_and(spared, offset < 0)))
        def _():
            for copy in relays(slot):
                copy.start()

        k = reach_at(t)

        @pl.when(jnp.logical_and(offset < 0, jnp.logical_not(early(k))))
        def _():
            for copy in sends(offset):
                copy.start()

    def weigh(slot):
        kinds = jnp.broadcast_to(spe[slot], (C, ATOMS)) == 1
        embedded = jnp.where(kinds, embb[1], embb[0])
        scaled = fea[slot].reshape(C, ATOMS) * embedded
        for n in range(NB):
            carr[:, n * ATOMS : (n + 1) * ATOMS] = (radb[n] * scaled).astype(BF)

    def product(tab, piece):
        at = slice(piece * 2 * ATOMS, min((piece + 1) * 2, NM) * ATOMS)
        acc[:, at] += jnp.dot(carr[...], tab[:, at], preferred_element_type=F32)

    def table(slot, apart, tab, between=None):
        other = jnp.concatenate([pos[slot], jnp.zeros((5, ATOMS), F32)], axis=0)
        columns = jnp.transpose(other)
        keep = maskb[slot]
        keep = jnp.concatenate([keep, keep], axis=0)
        for tile in range(ATOMS // HALF):
            if between is not None and tile < PIECES:
                product(between, tile)
            rows = slice(tile * HALF, (tile + 1) * HALF)
            dx = columns[rows, 0:1] - own_x
            dy = columns[rows, 1:2] - own_y
            dz = columns[rows, 2:3] - own_z
            dx = dx - box_x * jnp.floor(dx * (1.0 / box_x) + 0.5)
            dy = dy - cross_width * jnp.floor(dy * (1.0 / cross_width) + 0.5)
            dz = dz - cross_width * jnp.floor(dz * (1.0 / cross_width) + 0.5)
            square = dx * dx + dy * dy + dz * dz + soften
            inverse = lax.rsqrt(square)
            distance = square * inverse
            short = jnp.minimum(distance, cut_radius)
            x = short * (1.0 / cut_radius)
            x2 = x * x
            inner = x * (48.0 - 21.0 * x) - 28.0
            envelope = jnp.where(distance < cut_radius, 1.0 + x2 * x2 * x2 * inner, 0.0)
            same = (sublane + tile * HALF) == (lane + apart)
            amplitude = jnp.where(
                same, 0.0, (math.sqrt(2.0 / cut_radius) * inverse) * (envelope * keep)
            )
            sine, cosine = sin_cos(short * (math.pi / cut_radius))
            twice = 2.0 * cosine
            radial = [amplitude * sine]
            radial.append(twice * radial[0])
            for n in range(2, NB):
                radial.append(twice * radial[n - 1] - radial[n - 2])
            scale = inverse * root3
            hx, hy, hz = dx * scale, dy * scale, dz * scale
            gx, gy = ratio * hx, ratio * hy
            xx, yy = gx * hx, gy * hy
            zz = (2.0 * ratio) * (hz * hz)
            harmonics = [
                None,
                hx,
                hy,
                hz,
                gx * hy,
                gy * hz,
                (0.5 / root3) * (zz - xx - yy),
                gx * hz,
                0.5 * (xx - yy),
            ]
            for n in range(NB):
                at = slice(n * ATOMS + tile * HALF, n * ATOMS + (tile + 1) * HALF)
                for m in range(NM):
                    value = radial[n] if m == 0 else radial[n] * harmonics[m]
                    tab[at, m * ATOMS : (m + 1) * ATOMS] = value.astype(BF)

    def swapped(t):
        slot = offset_at(t) + HOPS

        @pl.when(t > 0)
        def _():
            arrived(fea.at[0, 0:2], fr.at[slot, 1])

        return slot

    def advance(t, tab, other_tab):
        fetch(t + 1)
        slot = swapped(t)
        weigh(slot)
        table(offset_at(t + 1) + HOPS, 2 * ATOMS, other_tab, tab)

    def finish(t, tab):
        weigh(swapped(t))
        for piece in range(PIECES):
            product(tab, piece)

    def side_of(i, carry):
        t = i * (HOPS + 1)

        @pl.when(i > 0)
        def _():
            fetch(t)

        table(offset_at(t) + HOPS, jnp.where(i == 0, 0, 2 * ATOMS), tab_a)
        advance(t, tab_a, tab_b)
        advance(t + 1, tab_b, tab_a)

        @pl.when(i == 0)
        def _():
            advance(t + 2, tab_a, tab_b)
            finish(t + 3, tab_b)

        @pl.when(i > 0)
        def _():
            finish(t + 2, tab_a)

        return carry

    lax.fori_loop(0, 2, side_of, 0)

    def sent(ref, sem):
        pltpu.make_async_remote_copy(
            src_ref=ref,
            dst_ref=ref,
            send_sem=sem,
            recv_sem=lsem.at[8],
            device_id={"blk": me, "chan": partner},
            device_id_type=MESH,
        ).wait_send()

    sent(fea.at[0:5], fs)
    sent(fea.at[0, 0], fs)

    @pl.when(jnp.logical_not(spared))
    def _():
        sent(fea.at[0:1], fs)
        sent(fea.at[0, 0:2], fs)

    @pl.when(directs)
    def _():
        sent(fea.at[0, 0], fs)

    sent(pos.at[0 : 2 * HOPS], ps)
    sent(spe.at[0 : 2 * HOPS], ss)
    sent(prm.at[0:3], qs)

    kinds = jnp.broadcast_to(spe[HOPS], (C, ATOMS)) == 1
    centre = jnp.where(kinds, embb[3], embb[2])
    order_of = (0, 1, 1, 1, 2, 2, 2, 2, 2)
    sums = [None, None, None]
    weights = []
    for order in range(3):
        w = mix[order]
        high = w.astype(BF)
        low = (w - high.astype(F32)).astype(BF)
        weights.append((high, low))
    for m in range(NM):
        f = acc[:, m * ATOMS : (m + 1) * ATOMS] * centre
        high = f.astype(BF)
        low = (f - high.astype(F32)).astype(BF)
        w_high, w_low = weights[order_of[m]]
        mixed = (
            jnp.dot(w_high, high, preferred_element_type=F32)
            + jnp.dot(w_low, high, preferred_element_type=F32)
            + jnp.dot(w_high, low, preferred_element_type=F32)
        )
        square = mixed * mixed
        order = order_of[m]
        sums[order] = square if sums[order] is None else sums[order] + square
    for order in range(3):
        out_ref[order] = sums[order]


def shards(
    positions,
    species,
    node_features,
    block_mask,
    radial_weight,
    species_embed,
    center_embed,
    mix_weight,
):
    n_blk = lax.axis_size("blk")
    box_x = float(n_blk) * slab_width
    dma = pltpu.SemaphoreType.DMA
    slots = 2 * HOPS + 1
    vmem = pltpu.VMEM
    sums = pl.pallas_call(
        functools.partial(kernel, box_x, n_blk, 8),
        name="pair_descriptor",
        out_shape=pltpu.VMEM((3, CD, ATOMS), F32),
        in_specs=[pl.BlockSpec(memory_space=pl.ANY)] * 8,
        out_specs=pl.BlockSpec(memory_space=pltpu.VMEM),
        scratch_shapes=[
            vmem((slots, 3, ATOMS), F32),
            vmem((slots, 1, ATOMS), jnp.int32),
            vmem((slots, CHANS, CD, ATOMS), F32),
            vmem((1, slots), jnp.int32),
            vmem((CHANS, 3, NB, CD), F32),
            vmem((3, CD, C), F32),
            vmem((slots, 8, ATOMS), F32),
            vmem((NB, C, ATOMS), F32),
            vmem((4, C, ATOMS), F32),
            vmem((NB * ATOMS, NM * ATOMS), BF),
            vmem((NB * ATOMS, NM * ATOMS), BF),
            vmem((C, NB * ATOMS), BF),
            vmem((C, NM * ATOMS), F32),
            dma((9,)),
            dma(()),
            dma((slots, 2)),
            dma(()),
            dma((slots,)),
            dma(()),
            dma((slots,)),
            dma(()),
            dma(()),
        ],
        compiler_params=pltpu.CompilerParams(collective_id=0, has_side_effects=True),
    )(
        positions,
        species.reshape(1, ATOMS),
        node_features,
        block_mask,
        radial_weight,
        species_embed.T,
        center_embed.T,
        mix_weight,
    )
    return jnp.log1p(sums)


def solution(mesh):
    return jax.shard_map(
        shards,
        mesh=mesh,
        in_specs=(
            P(None, "blk"),
            P("blk"),
            P("chan", "blk"),
            P("blk", None),
            P(None, "chan"),
            P("chan", None),
            P("chan", None),
            P(),
        ),
        out_specs=P(None, "chan", "blk"),
        check_vma=False,
    )
```

```python
import functools
import math

import jax
import jax.numpy as jnp
from jax import lax
from jax.experimental import pallas as pl
from jax.experimental.pallas import tpu as pltpu
from jax.sharding import PartitionSpec as P

MESH = pl.DeviceIdType.MESH

slab_width = 5.0 / 3.0
cross_width = 48.0
cut_radius = 5.0
soften = 0.25

HOPS = 3
ATOMS = 128
CHANS = 4
CD = 16
C = 64
NB = 8
NM = 9
HALF = 16
PIECES = 5
BF = jnp.bfloat16
F32 = jnp.float32


def sin_cos(angle):
    x = angle - 0.5 * math.pi
    y = x * x
    even = 2.0876756987868099e-9 * y - 2.755731922398589e-7
    even = even * y + 2.48015873015873e-5
    even = even * y - 1.388888888888889e-3
    even = even * y + 4.1666666666666664e-2
    even = even * y - 0.5
    even = even * y + 1.0
    odd = -2.505210838544172e-8 * y + 2.7557319223985893e-6
    odd = odd * y - 1.984126984126984e-4
    odd = odd * y + 8.333333333333333e-3
    odd = odd * y - 1.6666666666666666e-1
    odd = odd * y * x + x
    return even, -odd


def kernel(
    box_x,
    n_blk,
    row,
    pos_hbm,
    spe_hbm,
    fea_hbm,
    msk_hbm,
    rad_hbm,
    sem_hbm,
    cem_hbm,
    mix_hbm,
    out_ref,
    pos,
    spe,
    fea,
    msk,
    prm,
    mix,
    split,
    maskb,
    radb,
    embb,
    tab_a,
    tab_b,
    carr,
    acc,
    lsem,
    fs,
    fr,
    ps,
    pr,
    ss,
    sr,
    qs,
    qr,
):
    me = lax.axis_index("blk")
    ch = lax.axis_index("chan")
    last = n_blk - HOPS
    late = me >= last
    side = jnp.where(jnp.logical_and(lax.rem(me, row) < row // 2, me < last - HOPS), 1, -1)
    partner = ch + 1 - 2 * lax.rem(ch, 2)

    def slab(offset):
        return lax.rem(me + offset + n_blk, n_blk)

    def chan(c):
        return lax.rem(ch + c, CHANS)

    def to(offset, c):
        return {"blk": slab(offset), "chan": chan(c)}

    barrier = pltpu.get_barrier_semaphore()

    def greet(offset, c):
        pl.semaphore_signal(barrier, inc=1, device_id=to(offset, c), device_id_type=MESH)

    first = [
        pltpu.make_async_copy(pos_hbm, pos.at[HOPS], lsem.at[0]),
        pltpu.make_async_copy(spe_hbm, spe.at[HOPS], lsem.at[1]),
        pltpu.make_async_copy(fea_hbm, fea.at[HOPS, ch], lsem.at[2]),
    ]
    params = [
        pltpu.make_async_copy(rad_hbm, prm.at[ch, 0], lsem.at[3]),
        pltpu.make_async_copy(sem_hbm, prm.at[ch, 1, 0:2], lsem.at[4]),
        pltpu.make_async_copy(cem_hbm, prm.at[ch, 2, 0:2], lsem.at[5]),
    ]
    rest = [
        pltpu.make_async_copy(msk_hbm, msk, lsem.at[6]),
        pltpu.make_async_copy(
            mix_hbm.at[:, pl.ds(pl.multiple_of(ch * CD, CD), CD), :], mix, lsem.at[7]
        ),
    ]
    for copy in first:
        copy.start()

    even_late = jnp.logical_and(late, lax.rem(ch, 2) == 0)
    served = jnp.logical_and(me == 0, ch == 0)
    lone = jnp.logical_and(me == 0, ch == 1)

    ahead = jnp.logical_and(late, ch < 2)

    def apart_in_z(c):
        return chan(c) // 2 != ch // 2

    for k in (3, 2, 1):
        greet(-k, 0)
        greet(-k, 2)

    @pl.when(lone)
    def _():
        for k in (3, 2, 1):
            greet(-k, 1)
            greet(-k, 3)

    for c in (1, 2, 3):

        @pl.when(jnp.logical_not(jnp.logical_and(late, jnp.logical_and(ch >= 2, apart_in_z(c)))))
        def _(c=c):
            greet(0, c)

    for k in (1, 2, 3):

        @pl.when(me + k < last + (k >= HOPS))
        def _(k=k):
            greet(k, 0)
            greet(k, 2)

    for copy in params + rest:
        copy.start()
    for copy in first:
        copy.wait()
    lower = jnp.where(late, jnp.where(me == last, 1, 0), jnp.minimum(me, HOPS))
    straights = even_late.astype(jnp.int32)
    pl.semaphore_wait(barrier, jnp.where(ahead, 1, 3) + 2 * (HOPS + lower) + straights)

    def sends(offset):
        slot = HOPS - offset
        out = []
        for ref, sem, got in ((pos, ps, pr), (spe, ss, sr)):
            out.append(
                pltpu.make_async_remote_copy(
                    src_ref=ref.at[HOPS],
                    dst_ref=ref.at[slot],
                    send_sem=sem,
                    recv_sem=got.at[slot],
                    device_id=to(offset, 0),
                    device_id_type=MESH,
                )
            )
        lower_chip = jnp.where(ch >= 2, 2, 0)
        for c in (lower_chip, 2 - lower_chip):
            out.append(
                pltpu.make_async_remote_copy(
                    src_ref=fea.at[HOPS, ch],
                    dst_ref=fea.at[slot, ch],
                    send_sem=fs,
                    recv_sem=fr.at[slot, 0],
                    device_id=to(offset, c),
                    device_id_type=MESH,
                )
            )
        return out

    nearest = jnp.where(late, n_blk - me, HOPS)

    def direct(target):
        slot = HOPS - nearest
        return pltpu.make_async_remote_copy(
            src_ref=fea.at[HOPS, ch],
            dst_ref=fea.at[slot, ch],
            send_sem=fs,
            recv_sem=fr.at[slot, 1],
            device_id={"blk": 0, "chan": target},
            device_id_type=MESH,
        )

    @pl.when(even_late)
    def _():
        direct(1).start()

    for turn in range(HOPS):
        k = nearest + turn
        for copy in sends(jnp.where(k > HOPS, k - HOPS, k)):
            copy.start()

    def early(k):
        return jnp.logical_and(me >= k, me < jnp.where(k >= HOPS, last + 1, last))

    for k in (1, 2, 3):

        @pl.when(early(k))
        def _(k=k):
            for copy in sends(-k):
                copy.start()

    for copy in params:
        copy.wait()

    def gathers(c):
        out = []
        for ref, sem, got in (
            (prm.at[ch], qs, qr),
            (fea.at[HOPS, ch], fs, fr.at[HOPS, 0]),
        ):
            out.append(
                pltpu.make_async_remote_copy(
                    src_ref=ref,
                    dst_ref=ref,
                    send_sem=sem,
                    recv_sem=got,
                    device_id=to(0, c),
                    device_id_type=MESH,
                )
            )
        return out

    for c in (1, 2, 3):

        @pl.when(jnp.logical_not(jnp.logical_and(ahead, apart_in_z(c))))
        def _(c=c):
            for copy in gathers(c):
                copy.start()

    def relays(slot):
        out = []
        for q, c in ((0, 0), (1, 2)):
            a = chan(c)
            out.append(
                pltpu.make_async_remote_copy(
                    src_ref=fea.at[slot, a],
                    dst_ref=fea.at[slot, a],
                    send_sem=fs,
                    recv_sem=fr.at[slot, 1],
                    device_id={"blk": me, "chan": partner},
                    device_id_type=MESH,
                )
            )
        return out

    def arrived(ref, sem):
        pltpu.make_async_remote_copy(
            src_ref=ref,
            dst_ref=ref,
            send_sem=lsem.at[8],
            recv_sem=sem,
            device_id={"blk": me, "chan": partner},
            device_id_type=MESH,
        ).wait_recv()

    for copy in rest:
        copy.wait()
    for order in range(3):
        w = mix[order]
        high = w.astype(BF)
        split[order, :, 0:C] = high
        split[order, :, C : 2 * C] = (w - high.astype(F32)).astype(BF)
        split[order, :, 2 * C : 3 * C] = high
    for s in range(2 * HOPS + 1):
        maskb[s] = jnp.broadcast_to(msk[:, s : s + 1].astype(F32), (8, ATOMS))

    arrived(prm.at[0:3], qr)
    arrived(fea.at[0, 0:3], fr.at[HOPS, 0])
    for c in (1, 2, 3):

        @pl.when(jnp.logical_and(ahead, apart_in_z(c)))
        def _(c=c):
            for copy in gathers(c):
                copy.start()

    eye = lax.broadcasted_iota(jnp.int32, (CD, CD), 0) == lax.broadcasted_iota(
        jnp.int32, (CD, CD), 1
    )
    for q in range(CHANS):
        rows = slice(q * CD, (q + 1) * CD)
        for n in range(NB):
            row = jnp.broadcast_to(prm[q, 0, n : n + 1, :], (CD, CD))
            column = jnp.sum(jnp.where(eye, row, 0.0), axis=1, keepdims=True)
            radb[n, rows, :] = jnp.broadcast_to(column, (CD, ATOMS))
        for kind in (0, 1):
            for at, of in ((kind, 1), (2 + kind, 2)):
                row = jnp.broadcast_to(prm[q, of, kind : kind + 1, :], (CD, CD))
                column = jnp.sum(jnp.where(eye, row, 0.0), axis=1, keepdims=True)
                embb[at, rows, :] = jnp.broadcast_to(column, (CD, ATOMS))

    acc[...] = jnp.zeros_like(acc)
    own = pos[HOPS]
    own_x, own_y, own_z = own[0:1], own[1:2], own[2:3]
    lane = lax.broadcasted_iota(jnp.int32, (HALF, ATOMS), 1)
    sublane = lax.broadcasted_iota(jnp.int32, (HALF, ATOMS), 0)
    root3 = math.sqrt(3.0)
    ratio = math.sqrt(5.0 / 3.0)

    def reach_at(t):
        return jnp.where(jnp.logical_and(late, t <= HOPS), HOPS + 1 - t, lax.rem(t + 2, 3) + 1)

    def offset_at(t):
        k = reach_at(t)
        return jnp.where(t == 0, 0, jnp.where(t <= HOPS, side, -side) * k)

    def placed(t):
        slot = offset_at(t) + HOPS
        arrived(pos.at[slot], pr.at[slot])

    def fetch(t):
        placed(t)
        fill(t)

    def fill(t):
        offset = offset_at(t)
        slot = offset + HOPS
        arrived(spe.at[slot], sr.at[slot])
        arrived(fea.at[0, 0:2], fr.at[slot, 0])

        @pl.when(jnp.logical_not(jnp.logical_and(served, offset < 0)))
        def _():
            for copy in relays(slot):
                copy.start()

        k = reach_at(t)

        @pl.when(jnp.logical_and(offset < 0, jnp.logical_not(early(k))))
        def _():
            for copy in sends(offset):
                copy.start()

    def weigh(slot):
        kinds = jnp.broadcast_to(spe[slot], (C, ATOMS)) == 1
        embedded = jnp.where(kinds, embb[1], embb[0])
        scaled = fea[slot].reshape(C, ATOMS) * embedded
        for n in range(NB):
            carr[:, n * ATOMS : (n + 1) * ATOMS] = (radb[n] * scaled).astype(BF)

    def product(tab, piece):
        at = slice(piece * 2 * ATOMS, min((piece + 1) * 2, NM) * ATOMS)
        acc[:, at] += jnp.dot(carr[...], tab[:, at], preferred_element_type=F32)

    def table(slot, apart, tab, between=None):
        other = jnp.concatenate([pos[slot], jnp.zeros((5, ATOMS), F32)], axis=0)
        columns = jnp.transpose(other)
        keep = maskb[slot]
        keep = jnp.concatenate([keep, keep], axis=0)
        for tile in range(ATOMS // HALF):
            if between is not None and tile < PIECES:
                product(between, tile)
            rows = slice(tile * HALF, (tile + 1) * HALF)
            dx = columns[rows, 0:1] - own_x
            dy = columns[rows, 1:2] - own_y
            dz = columns[rows, 2:3] - own_z
            dx = dx - box_x * jnp.floor(dx * (1.0 / box_x) + 0.5)
            dy = dy - cross_width * jnp.floor(dy * (1.0 / cross_width) + 0.5)
            dz = dz - cross_width * jnp.floor(dz * (1.0 / cross_width) + 0.5)
            square = dx * dx + dy * dy + dz * dz + soften
            inverse = lax.rsqrt(square)
            distance = square * inverse
            short = jnp.minimum(distance, cut_radius)
            x = short * (1.0 / cut_radius)
            x2 = x * x
            inner = x * (48.0 - 21.0 * x) - 28.0
            envelope = jnp.where(distance < cut_radius, 1.0 + x2 * x2 * x2 * inner, 0.0)
            same = (sublane + tile * HALF) == (lane + apart)
            amplitude = jnp.where(
                same, 0.0, (math.sqrt(2.0 / cut_radius) * inverse) * (envelope * keep)
            )
            sine, cosine = sin_cos(short * (math.pi / cut_radius))
            twice = 2.0 * cosine
            radial = [amplitude * sine]
            radial.append(twice * radial[0])
            for n in range(2, NB):
                radial.append(twice * radial[n - 1] - radial[n - 2])
            scale = inverse * root3
            hx, hy, hz = dx * scale, dy * scale, dz * scale
            gx, gy = ratio * hx, ratio * hy
            xx, yy = gx * hx, gy * hy
            zz = (2.0 * ratio) * (hz * hz)
            harmonics = [
                None,
                hx,
                hy,
                hz,
                gx * hy,
                gy * hz,
                (0.5 / root3) * (zz - xx - yy),
                gx * hz,
                0.5 * (xx - yy),
            ]
            for n in range(NB):
                at = slice(n * ATOMS + tile * HALF, n * ATOMS + (tile + 1) * HALF)
                for m in range(NM):
                    value = radial[n] if m == 0 else radial[n] * harmonics[m]
                    tab[at, m * ATOMS : (m + 1) * ATOMS] = value.astype(BF)

    def swapped(t):
        slot = offset_at(t) + HOPS

        @pl.when(t > 0)
        def _():
            arrived(fea.at[0, 0:2], fr.at[slot, 1])

        return slot

    def advance(t, tab, other_tab):
        fetch(t + 1)
        slot = swapped(t)
        weigh(slot)
        table(offset_at(t + 1) + HOPS, 2 * ATOMS, other_tab, tab)

    def finish(t, tab):
        weigh(swapped(t))
        for piece in range(PIECES):
            product(tab, piece)

    def side_of(i, carry):
        t = i * (HOPS + 1)

        @pl.when(i > 0)
        def _():
            fetch(t)

        table(offset_at(t) + HOPS, jnp.where(i == 0, 0, 2 * ATOMS), tab_a)
        advance(t, tab_a, tab_b)
        alone = jnp.logical_and(lone, i > 0)

        @pl.when(jnp.logical_not(alone))
        def _():
            advance(t + 1, tab_b, tab_a)

        @pl.when(alone)
        def _():
            finish(t + 1, tab_b)
            placed(t + 2)
            table(offset_at(t + 2) + HOPS, 2 * ATOMS, tab_a)
            fill(t + 2)

        @pl.when(i == 0)
        def _():
            advance(t + 2, tab_a, tab_b)
            finish(t + 3, tab_b)

        @pl.when(i > 0)
        def _():
            finish(t + 2, tab_a)

        return carry

    lax.fori_loop(0, 2, side_of, 0)

    kinds = jnp.broadcast_to(spe[HOPS], (C, ATOMS)) == 1
    centre = jnp.where(kinds, embb[3], embb[2])
    for order, (start, stop) in enumerate(((0, 1), (1, 4), (4, 9))):
        at = slice(start * ATOMS, stop * ATOMS)
        f = acc[:, at] * jnp.concatenate([centre] * (stop - start), axis=1)
        high = f.astype(BF)
        low = (f - high.astype(F32)).astype(BF)
        mixed = jnp.dot(
            split[order], jnp.concatenate([high, high, low], axis=0), preferred_element_type=F32
        )
        square = mixed * mixed
        total = square[:, 0:ATOMS]
        for m in range(1, stop - start):
            total = total + square[:, m * ATOMS : (m + 1) * ATOMS]
        out_ref[order] = total

    def sent(ref, sem):
        pltpu.make_async_remote_copy(
            src_ref=ref,
            dst_ref=ref,
            send_sem=sem,
            recv_sem=lsem.at[8],
            device_id={"blk": me, "chan": partner},
            device_id_type=MESH,
        ).wait_send()

    sent(fea.at[0:5], fs)
    sent(fea.at[0, 0], fs)
    sent(pos.at[0 : 2 * HOPS], ps)
    sent(spe.at[0 : 2 * HOPS], ss)
    sent(prm.at[0:3], qs)

    @pl.when(jnp.logical_not(served))
    def _():
        sent(fea.at[0], fs)
        sent(fea.at[0, 0:2], fs)

    @pl.when(even_late)
    def _():
        sent(fea.at[0, 0], fs)


def shards(
    positions,
    species,
    node_features,
    block_mask,
    radial_weight,
    species_embed,
    center_embed,
    mix_weight,
):
    n_blk = lax.axis_size("blk")
    box_x = float(n_blk) * slab_width
    dma = pltpu.SemaphoreType.DMA
    slots = 2 * HOPS + 1
    vmem = pltpu.VMEM
    sums = pl.pallas_call(
        functools.partial(kernel, box_x, n_blk, 8),
        name="pair_descriptor",
        out_shape=pltpu.VMEM((3, CD, ATOMS), F32),
        in_specs=[pl.BlockSpec(memory_space=pl.ANY)] * 8,
        out_specs=pl.BlockSpec(memory_space=pltpu.VMEM),
        scratch_shapes=[
            vmem((slots, 3, ATOMS), F32),
            vmem((slots, 1, ATOMS), jnp.int32),
            vmem((slots, CHANS, CD, ATOMS), F32),
            vmem((1, slots), jnp.int32),
            vmem((CHANS, 3, NB, CD), F32),
            vmem((3, CD, C), F32),
            vmem((3, CD, 3 * C), BF),
            vmem((slots, 8, ATOMS), F32),
            vmem((NB, C, ATOMS), F32),
            vmem((4, C, ATOMS), F32),
            vmem((NB * ATOMS, NM * ATOMS), BF),
            vmem((NB * ATOMS, NM * ATOMS), BF),
            vmem((C, NB * ATOMS), BF),
            vmem((C, NM * ATOMS), F32),
            dma((9,)),
            dma(()),
            dma((slots, 2)),
            dma(()),
            dma((slots,)),
            dma(()),
            dma((slots,)),
            dma(()),
            dma(()),
        ],
        compiler_params=pltpu.CompilerParams(collective_id=0, has_side_effects=True),
    )(
        positions,
        species.reshape(1, ATOMS),
        node_features,
        block_mask,
        radial_weight,
        species_embed.T,
        center_embed.T,
        mix_weight,
    )
    return jnp.log1p(sums)


def solution(mesh):
    return jax.shard_map(
        shards,
        mesh=mesh,
        in_specs=(
            P(None, "blk"),
            P("blk"),
            P("chan", "blk"),
            P("blk", None),
            P(None, "chan"),
            P("chan", None),
            P("chan", None),
            P(),
        ),
        out_specs=P(None, "chan", "blk"),
        check_vma=False,
    )
```

```python
import functools
import math

import jax
import jax.numpy as jnp
from jax import lax
from jax.experimental import pallas as pl
from jax.experimental.pallas import tpu as pltpu
from jax.sharding import PartitionSpec as P

MESH = pl.DeviceIdType.MESH

slab_width = 5.0 / 3.0
cross_width = 48.0
cut_radius = 5.0
soften = 0.25

HOPS = 3
ATOMS = 128
CHANS = 4
CD = 16
C = 64
NB = 8
NM = 9
HALF = 16
PIECES = 5
BF = jnp.bfloat16
F32 = jnp.float32


def sin_cos(angle):
    x = angle - 0.5 * math.pi
    y = x * x
    even = 2.0876756987868099e-9 * y - 2.755731922398589e-7
    even = even * y + 2.48015873015873e-5
    even = even * y - 1.388888888888889e-3
    even = even * y + 4.1666666666666664e-2
    even = even * y - 0.5
    even = even * y + 1.0
    odd = -2.505210838544172e-8 * y + 2.7557319223985893e-6
    odd = odd * y - 1.984126984126984e-4
    odd = odd * y + 8.333333333333333e-3
    odd = odd * y - 1.6666666666666666e-1
    odd = odd * y * x + x
    return even, -odd


def kernel(
    box_x,
    n_blk,
    row,
    pos_hbm,
    spe_hbm,
    fea_hbm,
    msk_hbm,
    rad_hbm,
    sem_hbm,
    cem_hbm,
    mix_hbm,
    out_ref,
    pos,
    spe,
    fea,
    msk,
    prm,
    mix,
    split,
    maskb,
    radb,
    embb,
    tab_a,
    tab_b,
    carr,
    acc,
    lsem,
    fs,
    fr,
    ps,
    pr,
    ss,
    sr,
    qs,
    qr,
):
    me = lax.axis_index("blk")
    ch = lax.axis_index("chan")
    last = n_blk - HOPS
    late = me >= last
    side = jnp.where(jnp.logical_and(lax.rem(me, row) < row // 2, me < last - HOPS), 1, -1)
    partner = ch + 1 - 2 * lax.rem(ch, 2)

    def slab(offset):
        return lax.rem(me + offset + n_blk, n_blk)

    def chan(c):
        return lax.rem(ch + c, CHANS)

    def to(offset, c):
        return {"blk": slab(offset), "chan": chan(c)}

    barrier = pltpu.get_barrier_semaphore()

    def greet(offset, c):
        pl.semaphore_signal(barrier, inc=1, device_id=to(offset, c), device_id_type=MESH)

    first = [
        pltpu.make_async_copy(pos_hbm, pos.at[HOPS], lsem.at[0]),
        pltpu.make_async_copy(spe_hbm, spe.at[HOPS], lsem.at[1]),
        pltpu.make_async_copy(fea_hbm, fea.at[HOPS, ch], lsem.at[2]),
    ]
    params = [
        pltpu.make_async_copy(rad_hbm, prm.at[ch, 0], lsem.at[3]),
        pltpu.make_async_copy(sem_hbm, prm.at[ch, 1, 0:2], lsem.at[4]),
        pltpu.make_async_copy(cem_hbm, prm.at[ch, 2, 0:2], lsem.at[5]),
    ]
    rest = [
        pltpu.make_async_copy(msk_hbm, msk, lsem.at[6]),
        pltpu.make_async_copy(
            mix_hbm.at[:, pl.ds(pl.multiple_of(ch * CD, CD), CD), :], mix, lsem.at[7]
        ),
    ]
    for copy in first:
        copy.start()

    even_late = jnp.logical_and(late, lax.rem(ch, 2) == 0)
    served = jnp.logical_and(me == 0, ch == 0)
    lone = jnp.logical_and(me == 0, ch == 1)

    ahead = jnp.logical_and(late, ch < 2)

    def apart_in_z(c):
        return chan(c) // 2 != ch // 2

    def crossing(offset):
        return jnp.logical_and(late, jnp.logical_and(me + offset >= last, me + offset < n_blk))

    for k in (3, 2, 1):
        greet(-k, 0)

        @pl.when(jnp.logical_not(crossing(-k)))
        def _(k=k):
            greet(-k, 2)

    @pl.when(lone)
    def _():
        for k in (3, 2, 1):
            greet(-k, 1)
            greet(-k, 3)

    for c in (1, 2, 3):

        @pl.when(jnp.logical_not(jnp.logical_and(late, jnp.logical_and(ch >= 2, apart_in_z(c)))))
        def _(c=c):
            greet(0, c)

    for k in (1, 2, 3):

        @pl.when(me + k < last)
        def _(k=k):
            greet(k, 0)
            greet(k, 2)

    for copy in params + rest:
        copy.start()
    for copy in first:
        copy.wait()
    lower = jnp.where(late, 0, jnp.minimum(me, HOPS))
    straights = even_late.astype(jnp.int32)
    pl.semaphore_wait(barrier, jnp.where(ahead, 1, 3) + 2 * (HOPS + lower) + straights - jnp.where(late, n_blk - 1 - me, 0))

    def sends(offset):
        slot = HOPS - offset
        out = []
        for ref, sem, got in ((pos, ps, pr), (spe, ss, sr)):
            out.append(
                pltpu.make_async_remote_copy(
                    src_ref=ref.at[HOPS],
                    dst_ref=ref.at[slot],
                    send_sem=sem,
                    recv_sem=got.at[slot],
                    device_id=to(offset, 0),
                    device_id_type=MESH,
                )
            )
        for c in (0, 2):
            out.append(
                pltpu.make_async_remote_copy(
                    src_ref=fea.at[HOPS, ch],
                    dst_ref=fea.at[slot, ch],
                    send_sem=fs,
                    recv_sem=fr.at[slot, 0],
                    device_id=to(offset, c),
                    device_id_type=MESH,
                )
            )
        return out

    def begin(offset):
        copies = sends(offset)
        for copy in copies[:3]:
            copy.start()

        @pl.when(jnp.logical_not(crossing(offset)))
        def _():
            copies[3].start()

    nearest = jnp.where(late, n_blk - me, HOPS)

    def direct(target):
        slot = HOPS - nearest
        return pltpu.make_async_remote_copy(
            src_ref=fea.at[HOPS, ch],
            dst_ref=fea.at[slot, ch],
            send_sem=fs,
            recv_sem=fr.at[slot, 1],
            device_id={"blk": 0, "chan": target},
            device_id_type=MESH,
        )

    @pl.when(even_late)
    def _():
        direct(1).start()

    for turn in range(HOPS):
        k = nearest + turn
        begin(jnp.where(k > HOPS, k - HOPS, k))

    def early(k):
        return jnp.logical_and(me >= k, me < last)

    for k in (1, 2, 3):

        @pl.when(early(k))
        def _(k=k):
            begin(-k)

    for copy in params:
        copy.wait()

    def gathers(c):
        out = []
        for ref, sem, got in (
            (prm.at[ch], qs, qr),
            (fea.at[HOPS, ch], fs, fr.at[HOPS, 0]),
        ):
            out.append(
                pltpu.make_async_remote_copy(
                    src_ref=ref,
                    dst_ref=ref,
                    send_sem=sem,
                    recv_sem=got,
                    device_id=to(0, c),
                    device_id_type=MESH,
                )
            )
        return out

    for c in (1, 2, 3):

        @pl.when(jnp.logical_not(jnp.logical_and(ahead, apart_in_z(c))))
        def _(c=c):
            for copy in gathers(c):
                copy.start()

    def relays(slot):
        out = []
        for q, c in ((0, 0), (1, 2)):
            a = chan(c)
            out.append(
                pltpu.make_async_remote_copy(
                    src_ref=fea.at[slot, a],
                    dst_ref=fea.at[slot, a],
                    send_sem=fs,
                    recv_sem=fr.at[slot, 1],
                    device_id={"blk": me, "chan": partner},
                    device_id_type=MESH,
                )
            )
        return out

    def arrived(ref, sem):
        pltpu.make_async_remote_copy(
            src_ref=ref,
            dst_ref=ref,
            send_sem=lsem.at[8],
            recv_sem=sem,
            device_id={"blk": me, "chan": partner},
            device_id_type=MESH,
        ).wait_recv()

    for copy in rest:
        copy.wait()
    for order in range(3):
        w = mix[order]
        high = w.astype(BF)
        split[order, :, 0:C] = high
        split[order, :, C : 2 * C] = (w - high.astype(F32)).astype(BF)
        split[order, :, 2 * C : 3 * C] = high
    for s in range(2 * HOPS + 1):
        maskb[s] = jnp.broadcast_to(msk[:, s : s + 1].astype(F32), (8, ATOMS))

    arrived(prm.at[0:3], qr)
    arrived(fea.at[0, 0:3], fr.at[HOPS, 0])
    for c in (1, 2, 3):

        @pl.when(jnp.logical_and(ahead, apart_in_z(c)))
        def _(c=c):
            for copy in gathers(c):
                copy.start()

    eye = lax.broadcasted_iota(jnp.int32, (CD, CD), 0) == lax.broadcasted_iota(
        jnp.int32, (CD, CD), 1
    )
    for q in range(CHANS):
        rows = slice(q * CD, (q + 1) * CD)
        for n in range(NB):
            row = jnp.broadcast_to(prm[q, 0, n : n + 1, :], (CD, CD))
            column = jnp.sum(jnp.where(eye, row, 0.0), axis=1, keepdims=True)
            radb[n, rows, :] = jnp.broadcast_to(column, (CD, ATOMS))
        for kind in (0, 1):
            for at, of in ((kind, 1), (2 + kind, 2)):
                row = jnp.broadcast_to(prm[q, of, kind : kind + 1, :], (CD, CD))
                column = jnp.sum(jnp.where(eye, row, 0.0), axis=1, keepdims=True)
                embb[at, rows, :] = jnp.broadcast_to(column, (CD, ATOMS))

    acc[...] = jnp.zeros_like(acc)
    own = pos[HOPS]
    own_x, own_y, own_z = own[0:1], own[1:2], own[2:3]
    lane = lax.broadcasted_iota(jnp.int32, (HALF, ATOMS), 1)
    sublane = lax.broadcasted_iota(jnp.int32, (HALF, ATOMS), 0)
    root3 = math.sqrt(3.0)
    ratio = math.sqrt(5.0 / 3.0)

    def reach_at(t):
        return lax.rem(t + 2, 3) + 1

    def offset_at(t):
        k = reach_at(t)
        return jnp.where(t == 0, 0, jnp.where(t <= HOPS, side, -side) * k)

    def placed(t):
        slot = offset_at(t) + HOPS
        arrived(pos.at[slot], pr.at[slot])

    def fetch(t):
        placed(t)
        fill(t)

    def fill(t):
        offset = offset_at(t)
        slot = offset + HOPS
        arrived(spe.at[slot], sr.at[slot])
        swap = crossing(offset)
        k = reach_at(t)
        answers = jnp.logical_and(offset < 0, jnp.logical_not(early(k)))

        @pl.when(swap)
        def _():
            arrived(fea.at[0, 0], fr.at[slot, 0])

            @pl.when(answers)
            def _():
                begin(offset)

            pltpu.make_async_remote_copy(
                src_ref=fea.at[slot, ch],
                dst_ref=fea.at[slot, ch],
                send_sem=fs,
                recv_sem=fr.at[slot, 2],
                device_id=to(0, 2),
                device_id_type=MESH,
            ).start()
            arrived(fea.at[0, 0], fr.at[slot, 2])

        @pl.when(jnp.logical_not(swap))
        def _():
            arrived(fea.at[0, 0:2], fr.at[slot, 0])

            @pl.when(answers)
            def _():
                begin(offset)


        @pl.when(jnp.logical_not(jnp.logical_and(served, offset < 0)))
        def _():
            for copy in relays(slot):
                copy.start()


    def weigh(slot):
        kinds = jnp.broadcast_to(spe[slot], (C, ATOMS)) == 1
        embedded = jnp.where(kinds, embb[1], embb[0])
        scaled = fea[slot].reshape(C, ATOMS) * embedded
        for n in range(NB):
            carr[:, n * ATOMS : (n + 1) * ATOMS] = (radb[n] * scaled).astype(BF)

    def product(tab, piece):
        at = slice(piece * 2 * ATOMS, min((piece + 1) * 2, NM) * ATOMS)
        acc[:, at] += jnp.dot(carr[...], tab[:, at], preferred_element_type=F32)

    def table(slot, apart, tab, between=None):
        other = jnp.concatenate([pos[slot], jnp.zeros((5, ATOMS), F32)], axis=0)
        columns = jnp.transpose(other)
        keep = maskb[slot]
        keep = jnp.concatenate([keep, keep], axis=0)
        for tile in range(ATOMS // HALF):
            if between is not None and tile < PIECES:
                product(between, tile)
            rows = slice(tile * HALF, (tile + 1) * HALF)
            dx = columns[rows, 0:1] - own_x
            dy = columns[rows, 1:2] - own_y
            dz = columns[rows, 2:3] - own_z
            dx = dx - box_x * jnp.floor(dx * (1.0 / box_x) + 0.5)
            dy = dy - cross_width * jnp.floor(dy * (1.0 / cross_width) + 0.5)
            dz = dz - cross_width * jnp.floor(dz * (1.0 / cross_width) + 0.5)
            square = dx * dx + dy * dy + dz * dz + soften
            inverse = lax.rsqrt(square)
            distance = square * inverse
            short = jnp.minimum(distance, cut_radius)
            x = short * (1.0 / cut_radius)
            x2 = x * x
            inner = x * (48.0 - 21.0 * x) - 28.0
            envelope = jnp.where(distance < cut_radius, 1.0 + x2 * x2 * x2 * inner, 0.0)
            same = (sublane + tile * HALF) == (lane + apart)
            amplitude = jnp.where(
                same, 0.0, (math.sqrt(2.0 / cut_radius) * inverse) * (envelope * keep)
            )
            sine, cosine = sin_cos(short * (math.pi / cut_radius))
            twice = 2.0 * cosine
            radial = [amplitude * sine]
            radial.append(twice * radial[0])
            for n in range(2, NB):
                radial.append(twice * radial[n - 1] - radial[n - 2])
            scale = inverse * root3
            hx, hy, hz = dx * scale, dy * scale, dz * scale
            gx, gy = ratio * hx, ratio * hy
            xx, yy = gx * hx, gy * hy
            zz = (2.0 * ratio) * (hz * hz)
            harmonics = [
                None,
                hx,
                hy,
                hz,
                gx * hy,
                gy * hz,
                (0.5 / root3) * (zz - xx - yy),
                gx * hz,
                0.5 * (xx - yy),
            ]
            for n in range(NB):
                at = slice(n * ATOMS + tile * HALF, n * ATOMS + (tile + 1) * HALF)
                for m in range(NM):
                    value = radial[n] if m == 0 else radial[n] * harmonics[m]
                    tab[at, m * ATOMS : (m + 1) * ATOMS] = value.astype(BF)

    def swapped(t):
        slot = offset_at(t) + HOPS

        @pl.when(t > 0)
        def _():
            arrived(fea.at[0, 0:2], fr.at[slot, 1])

        return slot

    def advance(t, tab, other_tab):
        fetch(t + 1)
        slot = swapped(t)
        weigh(slot)
        table(offset_at(t + 1) + HOPS, 2 * ATOMS, other_tab, tab)

    def finish(t, tab):
        weigh(swapped(t))
        for piece in range(PIECES):
            product(tab, piece)

    def side_of(i, carry):
        t = i * (HOPS + 1)

        @pl.when(i > 0)
        def _():
            fetch(t)

        table(offset_at(t) + HOPS, jnp.where(i == 0, 0, 2 * ATOMS), tab_a)
        advance(t, tab_a, tab_b)
        alone = jnp.logical_and(lone, i > 0)

        @pl.when(jnp.logical_not(alone))
        def _():
            advance(t + 1, tab_b, tab_a)

        @pl.when(alone)
        def _():
            finish(t + 1, tab_b)
            placed(t + 2)
            table(offset_at(t + 2) + HOPS, 2 * ATOMS, tab_a)
            fill(t + 2)

        @pl.when(i == 0)
        def _():
            advance(t + 2, tab_a, tab_b)
            finish(t + 3, tab_b)

        @pl.when(i > 0)
        def _():
            finish(t + 2, tab_a)

        return carry

    lax.fori_loop(0, 2, side_of, 0)

    kinds = jnp.broadcast_to(spe[HOPS], (C, ATOMS)) == 1
    centre = jnp.where(kinds, embb[3], embb[2])
    for order, (start, stop) in enumerate(((0, 1), (1, 4), (4, 9))):
        at = slice(start * ATOMS, stop * ATOMS)
        f = acc[:, at] * jnp.concatenate([centre] * (stop - start), axis=1)
        high = f.astype(BF)
        low = (f - high.astype(F32)).astype(BF)
        mixed = jnp.dot(
            split[order], jnp.concatenate([high, high, low], axis=0), preferred_element_type=F32
        )
        square = mixed * mixed
        total = square[:, 0:ATOMS]
        for m in range(1, stop - start):
            total = total + square[:, m * ATOMS : (m + 1) * ATOMS]
        out_ref[order] = total

    def sent(ref, sem):
        pltpu.make_async_remote_copy(
            src_ref=ref,
            dst_ref=ref,
            send_sem=sem,
            recv_sem=lsem.at[8],
            device_id={"blk": me, "chan": partner},
            device_id_type=MESH,
        ).wait_send()

    sent(fea.at[0:5], fs)
    sent(fea.at[0, 0], fs)
    sent(pos.at[0 : 2 * HOPS], ps)
    sent(spe.at[0 : 2 * HOPS], ss)
    sent(prm.at[0:3], qs)

    @pl.when(jnp.logical_not(served))
    def _():
        sent(fea.at[0], fs)
        sent(fea.at[0, 0:2], fs)

    @pl.when(even_late)
    def _():
        sent(fea.at[0, 0], fs)


def shards(
    positions,
    species,
    node_features,
    block_mask,
    radial_weight,
    species_embed,
    center_embed,
    mix_weight,
):
    n_blk = lax.axis_size("blk")
    box_x = float(n_blk) * slab_width
    dma = pltpu.SemaphoreType.DMA
    slots = 2 * HOPS + 1
    vmem = pltpu.VMEM
    sums = pl.pallas_call(
        functools.partial(kernel, box_x, n_blk, 8),
        name="pair_descriptor",
        out_shape=pltpu.VMEM((3, CD, ATOMS), F32),
        in_specs=[pl.BlockSpec(memory_space=pl.ANY)] * 8,
        out_specs=pl.BlockSpec(memory_space=pltpu.VMEM),
        scratch_shapes=[
            vmem((slots, 3, ATOMS), F32),
            vmem((slots, 1, ATOMS), jnp.int32),
            vmem((slots, CHANS, CD, ATOMS), F32),
            vmem((1, slots), jnp.int32),
            vmem((CHANS, 3, NB, CD), F32),
            vmem((3, CD, C), F32),
            vmem((3, CD, 3 * C), BF),
            vmem((slots, 8, ATOMS), F32),
            vmem((NB, C, ATOMS), F32),
            vmem((4, C, ATOMS), F32),
            vmem((NB * ATOMS, NM * ATOMS), BF),
            vmem((NB * ATOMS, NM * ATOMS), BF),
            vmem((C, NB * ATOMS), BF),
            vmem((C, NM * ATOMS), F32),
            dma((9,)),
            dma(()),
            dma((slots, 3)),
            dma(()),
            dma((slots,)),
            dma(()),
            dma((slots,)),
            dma(()),
            dma(()),
        ],
        compiler_params=pltpu.CompilerParams(collective_id=0, has_side_effects=True),
    )(
        positions,
        species.reshape(1, ATOMS),
        node_features,
        block_mask,
        radial_weight,
        species_embed.T,
        center_embed.T,
        mix_weight,
    )
    return jnp.log1p(sums)


def solution(mesh):
    return jax.shard_map(
        shards,
        mesh=mesh,
        in_specs=(
            P(None, "blk"),
            P("blk"),
            P("chan", "blk"),
            P("blk", None),
            P(None, "chan"),
            P("chan", None),
            P("chan", None),
            P(),
        ),
        out_specs=P(None, "chan", "blk"),
        check_vma=False,
    )
```
